128 devices in a mesh: comp: 8 (over x_lo, y), dom: 16 (over z, x_hi, core).
Axes of the slice: x: 4 (x_hi: 2, x_lo: 2; x = x_hi * 2 + x_lo), y: 4, z: 4, core: 2. Of those that a mesh axis runs over, the one named last changes fastest.
Arguments:
- densities: float32 [8, 6144, 2048], P('comp', 'dom'), may hold values from -6 to 6
- levels: int32 [8, 2], P('comp'), may hold values from 0 to 3
- coeffs: int32 [8], P('comp'), may hold values from -1 to 1, as said below
Outputs:
- result: float32 [8, 6144, 2048], P('comp', 'dom')
The draws below stay inside these ranges and needn't reach their ends.
Inputs may be any that keep to these rules, and one draw needn't show every extreme that they name: `coeffs`: each coefficient is -1 or 1; both values occur.
All inputs are finite; a program needn't handle non-finite values.
Results may differ from the reference program's by a relative error of at most 0.0001.
Values sent between devices are 32-bit elements; how exact they have to be, the bound alone decides.
A program may use at most 64 MiB of HBM per device.

```python
import jax
import jax.numpy as jnp
from jax import lax

NV = 2048
MX = 2048
MV = 256
PRE = 8
POST = 2
GROUPS = 8
NX = 6144


def draw_coeffs(key, part):
    sign_key = jax.random.fold_in(key, 11)
    order_key = jax.random.fold_in(key, 23)
    signs = 2 * jax.random.randint(sign_key, (GROUPS,), 0, 2) - 1
    order = jax.random.permutation(order_key, GROUPS)
    fixed = jnp.where(order == 0, 1, jnp.where(order == 1, -1, signs))
    return fixed.astype(jnp.int32)


def plant(array, key, least, high):
    spot = [jax.random.randint(jax.random.fold_in(key, axis), (), 0, length) for axis, length in enumerate(array.shape)]
    main_axis = array.shape.index(max(array.shape))
    beside = spot[:main_axis] + [(spot[main_axis] + 1) % array.shape[main_axis]] + spot[main_axis + 1:]
    return array.at[tuple(spot)].set(least).at[tuple(beside)].set(high)


def block_scale(own_key, extent, pieces, low, top_value):
    factor_of, own = 1.0, jax.random.fold_in(own_key, 6)
    for axis_at, blocks in pieces:
        steps = jnp.exp(jax.random.uniform(jax.random.fold_in(own, axis_at), (blocks,), jnp.float32, low / len(pieces), top_value / len(pieces)))
        factor_of = factor_of * jnp.repeat(steps, extent[axis_at] // blocks).reshape([-1 if axis == axis_at else 1 for axis in range(len(extent))])
    return factor_of


def scatter_about(key, dims, deviation, limit, shards=(), kind=jnp.bfloat16):
    entries = jax.random.normal(key, dims, jnp.float32) * deviation
    if len(shards) > 0:
        entries = block_scale(key, dims, shards, -0.22, 0.18) * entries
    return jnp.clip(entries, min=-limit, max=limit).astype(kind)


def setup_inputs(seed: int = 0) -> dict:
    streams_of = jax.random.split(jax.random.key(seed), 4)
    return {
        "densities": scatter_about(streams_of[0], (GROUPS, NX, NV), 1.0, 6.0, ((0, 8), (1, 16)), jnp.float32),
        "levels": plant(jax.random.randint(streams_of[1], (GROUPS, 2), 0, 4), jax.random.fold_in(streams_of[1], 1), 0, 3).astype(jnp.int32),
        "coeffs": draw_coeffs(jax.random.fold_in(streams_of[3], 71), 0),
    }


HIGHEST_PRECISION = lax.Precision.HIGHEST

def cosine_basis(positions, mode_count, length):
    mode_ids = jnp.arange(mode_count, dtype=jnp.float32)
    phases = jnp.pi * (positions[:, None] + 0.5) * mode_ids[None, :] / length
    column_scale = jnp.where(mode_ids == 0, jnp.sqrt(1.0 / length), jnp.sqrt(2.0 / length))
    return jnp.cos(phases) * column_scale[None, :]

def damping(level, mode_count):
    mode_ids = jnp.arange(mode_count, dtype=jnp.float32)
    factor = jnp.exp2((3 - level).astype(jnp.float32))
    return 1.0 / (1.0 + (mode_ids * factor / mode_count) ** 2)

def advance(density, lower_rows, upper_rows, courant, diffusion, active):
    vel_cells = density.shape[1]
    velocity = -1.0 + (2.0 * jnp.arange(vel_cells, dtype=jnp.float32) + 1.0) / vel_cells
    upwind = jnp.where(velocity[None, :] > 0, density - lower_rows, upper_rows - density)
    padded_v = jnp.concatenate([density[:, :1], density, density[:, -1:]], axis=1)
    laplace = padded_v[:, 2:] - 2.0 * density + padded_v[:, :-2]
    return density - active * (courant * velocity[None, :] * upwind - diffusion * laplace)

def step_full(density, courant, diffusion, active):
    return advance(density, jnp.roll(density, 1, 0), jnp.roll(density, -1, 0), courant, diffusion, active)

def reference(densities, levels, coeffs):
    basis_x = cosine_basis(jnp.arange(NX, dtype=jnp.float32), MX, NX)
    basis_v = cosine_basis(jnp.arange(NV, dtype=jnp.float32), MV, NV)
    advanced_all = []
    surplus_all = []
    rates = []
    for group in range(GROUPS):
        level_x = levels[group, 0]
        level_v = levels[group, 1]
        courant = 0.3 + level_x.astype(jnp.float32) / 15.0
        diffusion = 0.1 + level_v.astype(jnp.float32) / 30.0
        density = densities[group]
        for step_id in range(PRE):
            active = (step_id < PRE - 3 + level_x).astype(jnp.float32)
            density = step_full(density, courant, diffusion, active)
        reduced = jnp.dot(density, basis_v, precision=HIGHEST_PRECISION)
        projected = jnp.dot(basis_x.T, reduced, precision=HIGHEST_PRECISION)
        own_surplus = damping(level_x, MX)[:, None] * projected * damping(level_v, MV)[None, :]
        advanced_all.append(density)
        surplus_all.append(own_surplus)
        rates.append((courant, diffusion))
    combined = jnp.zeros((MX, MV), jnp.float32)
    for group in range(GROUPS):
        combined = combined + coeffs[group].astype(jnp.float32) * surplus_all[group]
    outputs = []
    for group in range(GROUPS):
        courant, diffusion = rates[group]
        correction = jnp.dot(basis_x, combined - surplus_all[group], precision=HIGHEST_PRECISION)
        density = advanced_all[group] + jnp.dot(correction, basis_v.T, precision=HIGHEST_PRECISION)
        for step_id in range(POST):
            density = step_full(density, courant, diffusion, jnp.float32(1.0))
        outputs.append(density)
    return jnp.stack(outputs)
```

```python
import functools

import jax
import jax.numpy as jnp
import numpy as np
from jax import lax
from jax.experimental import pallas as pl
from jax.experimental.pallas import tpu as pltpu
from jax.sharding import PartitionSpec as P

MX = 2048
MV = 256
PRE = 8
POST = 2
NV = 2048
ROWS = 384
NX = 6144
LANES = 128
TILES = NV // LANES
HALO = 16
LEAD = 24
PLANE_ROWS = 432
WIDE = 400
NCH = 4
KC = MX // NCH
KQ = KC // 4
MESH = pl.DeviceIdType.MESH
F32 = jnp.float32
BF16 = jnp.bfloat16

TWO_PI_HI = float(np.float32(6.28125))
TWO_PI_LO = float(np.float32(2.0 * np.pi - 6.28125))
INV_TWO_PI = float(np.float32(1.0 / (2.0 * np.pi)))


def sine_terms():
    count = 6
    nodes = np.cos(np.pi * (np.arange(64) + 0.5) / 128)
    r = np.pi * nodes
    u = r * r
    basis = np.stack([u**i for i in range(count)], axis=1)
    target = np.sqrt(2.0) * np.sin(r / 2) / r
    terms, *_ = np.linalg.lstsq(basis * r[:, None], target * r, rcond=None)
    return [float(np.float32(t)) for t in terms]


SINE_TERMS = sine_terms()


def cosine(phase):
    turns = jnp.round(phase * INV_TWO_PI)
    r = (phase - turns * TWO_PI_HI) - turns * TWO_PI_LO
    u = r * r
    s = jnp.full_like(u, SINE_TERMS[-1])
    for term in SINE_TERMS[-2::-1]:
        s = s * u + term
    s = s * r
    return 1.0 - s * s


def split(x):
    hi = x.astype(BF16)
    return hi, (x - hi.astype(F32)).astype(BF16)


def dot3(a_hi, a_lo, b_hi, b_lo, dims):
    def dot(a, b):
        return lax.dot_general(a, b, (dims, ((), ())), preferred_element_type=F32)

    return dot(a_hi, b_hi) + dot(a_hi, b_lo) + dot(a_lo, b_hi)


NN = ((1,), (0,))
NT = ((1,), (1,))


def kernel(
    lev_ref,
    coef_ref,
    dens_ref,
    out_ref,
    fa,
    fb,
    al_ref,
    be_ref,
    bx_h,
    bx_l,
    bv_h,
    bv_l,
    red_h,
    red_l,
    part,
    core_in,
    core_sum,
    z1_in,
    z1_sum,
    z2_in,
    block,
    plane_in,
    back_out,
    upd,
    corr,
    coef_own,
    coef_all,
    in_sem,
    out_sem,
    halo_send,
    halo_recv,
    coef_send,
    coef_recv,
    core_send,
    core_recv,
    z1_send,
    z1_recv,
    z2_send,
    z2_recv,
    plane_send,
    plane_recv,
    back_send,
    back_recv,
    g2_send,
    g2_recv,
    g1_send,
    g1_recv,
    gc_send,
    gc_recv,
):
    c = lax.axis_index("comp")
    d = lax.axis_index("dom")
    z = d // 4
    xh = (d // 2) % 2
    core = d % 2
    p = c * 2 + xh
    nxt = (d + 1) % 16
    prv = (d + 15) % 16
    peer = d + 1 - 2 * core
    za = (z + 1 - 2 * (z % 2)) * 4 + d % 4
    zb = (3 - z) * 4 + d % 4
    s1 = (z % 2 + z // 2) % 2
    s2 = z // 2
    t1 = z // 2
    t2 = s1

    def dom_id(dom):
        return {"comp": c, "dom": dom}

    def plane_id(q):
        return {"comp": q // 2, "dom": z * 4 + (q % 2) * 2 + core}

    barrier = pltpu.get_barrier_semaphore()
    for dom in (nxt, prv, peer, za, zb):
        pl.semaphore_signal(barrier, inc=1, device_id=dom_id(dom), device_id_type=MESH)
    for o in range(1, 16):
        q = (p + o) % 16
        pl.semaphore_signal(barrier, inc=1, device_id=plane_id(q), device_id_type=MESH)

    def load(t):
        return pltpu.make_async_copy(
            dens_ref.at[0, :, pl.ds(t * LANES, LANES)],
            fa.at[t, pl.ds(LEAD, ROWS), :],
            in_sem.at[t],
        )

    for t in range(TILES):
        load(t).start()

    lev_x = lev_ref[0, 0]
    lev_v = lev_ref[0, 1]
    courant = 0.3 + lev_x.astype(F32) / 15.0
    diffusion = 0.1 + lev_v.astype(F32) / 30.0
    coef_own[...] = jnp.full((8, LANES), coef_ref[0].astype(F32), F32)
    coef_all[c] = coef_own[...]

    def power(level):
        return jnp.where(level == 0, 8.0, jnp.where(level == 1, 4.0, jnp.where(level == 2, 2.0, 1.0))).astype(F32)

    lane = lax.broadcasted_iota(jnp.int32, (16, LANES), 1)
    row16 = lax.broadcasted_iota(jnp.int32, (16, LANES), 0)

    def velocity_basis(i, _):
        mode = (row16 + i * 16).astype(F32)
        r0 = pl.multiple_of(i * 16, 16)
        for t in range(TILES):
            cell = (lane + t * LANES).astype(F32)
            phase = ((np.float32(np.pi) * (cell + 0.5)) * mode) * np.float32(1.0 / NV)
            hi, lo = split(cosine(phase))
            bv_h[pl.ds(r0, 16), t * LANES : (t + 1) * LANES] = hi
            bv_l[pl.ds(r0, 16), t * LANES : (t + 1) * LANES] = lo
        return 0

    lax.fori_loop(0, MV // 16, velocity_basis, 0)

    for t in range(TILES):
        load(t).wait()
    pl.semaphore_wait(barrier, 20)

    halo_up = pltpu.make_async_remote_copy(
        src_ref=fa.at[:, pl.ds(LEAD, HALO), :],
        dst_ref=fa.at[:, pl.ds(LEAD + ROWS, HALO), :],
        send_sem=halo_send.at[0],
        recv_sem=halo_recv.at[0],
        device_id=dom_id(prv),
        device_id_type=MESH,
    )
    halo_down = pltpu.make_async_remote_copy(
        src_ref=fa.at[:, pl.ds(LEAD + ROWS - HALO, HALO), :],
        dst_ref=fa.at[:, pl.ds(LEAD - HALO, HALO), :],
        send_sem=halo_send.at[1],
        recv_sem=halo_recv.at[1],
        device_id=dom_id(nxt),
        device_id_type=MESH,
    )
    halo_up.start()
    halo_down.start()

    def coef_copy(o):
        return pltpu.make_async_remote_copy(
            src_ref=coef_own,
            dst_ref=coef_all.at[c],
            send_sem=coef_send.at[o],
            recv_sem=coef_recv.at[o],
            device_id={"comp": (c + o) % 8, "dom": d},
            device_id_type=MESH,
        )

    for o in range(1, 8):
        coef_copy(o).start()

    def space_basis(i, _):
        local = row16 + i * 16
        local = jnp.where(local >= ROWS + 8, local - WIDE, local)
        cell = local + d * ROWS
        cell = jnp.where(cell < 0, cell + NX, cell)
        cell = jnp.where(cell >= NX, cell - NX, cell)
        angle = np.float32(np.pi) * (cell.astype(F32) + 0.5)
        r0 = pl.multiple_of(i * 16, 16)
        for t in range(TILES):
            mode = (lane + t * LANES).astype(F32)
            phase = (angle * mode) * np.float32(1.0 / NX)
            hi, lo = split(cosine(phase))
            bx_h[pl.ds(r0, 16), t * LANES : (t + 1) * LANES] = hi
            bx_l[pl.ds(r0, 16), t * LANES : (t + 1) * LANES] = lo
        return 0

    lax.fori_loop(0, WIDE // 16, space_basis, 0)

    lane8 = lax.broadcasted_iota(jnp.int32, (8, LANES), 1)

    def set_rates(active):
        for t in range(TILES):
            cell = (lane8 + t * LANES).astype(F32)
            speed = jnp.abs(-1.0 + (2.0 * cell + 1.0) / NV) * courant
            al_ref[t] = 1.0 - active * (2.0 * diffusion + speed)
            be_ref[t] = active * speed
        return active * diffusion

    first_lane = lane == 0
    last_lane = lane == LANES - 1

    def step(src, dst, start, count, rate):
        def rows(i, _):
            r = start + i * 16
            r8 = pl.multiple_of(r, 8)
            f = [src[t, pl.ds(r8, 16), :] for t in range(TILES)]
            rl = [pltpu.roll(x, 1, 1) for x in f]
            rr = [pltpu.roll(x, LANES - 1, 1) for x in f]
            for t in range(TILES):
                left = jnp.where(first_lane, rl[t - 1] if t > 0 else f[0], rl[t])
                right = jnp.where(last_lane, rr[t + 1] if t < TILES - 1 else f[t], rr[t])
                shifted = src[t, pl.ds(r + 1 if t < TILES // 2 else r - 1, 16), :]
                al = jnp.concatenate([al_ref[t]] * 2, axis=0)
                be = jnp.concatenate([be_ref[t]] * 2, axis=0)
                dst[t, pl.ds(r8, 16), :] = al * f[t] + be * shifted + rate * (left + right)
            return 0

        lax.fori_loop(0, count // 16, rows, 0)

    rate = set_rates(jnp.float32(1.0))
    halo_up.wait_recv()
    halo_down.wait_recv()
    halo_up.wait_send()
    halo_down.wait_send()
    src, dst = fa, fb
    for s in range(PRE):
        if s >= PRE - 3:
            rate = set_rates(jnp.where(lev_x > s - (PRE - 3), 1.0, 0.0).astype(F32))
        if s == 0:
            step(src, dst, LEAD - HALO, ROWS + 2 * HALO, rate)
        else:
            step(src, dst, LEAD - 8, WIDE, rate)
        src, dst = dst, src

    reduced = jnp.zeros((ROWS, MV), F32)
    for kt in range(TILES // 2):
        block_f = jnp.concatenate([fa[2 * kt, LEAD : LEAD + ROWS, :], fa[2 * kt + 1, LEAD : LEAD + ROWS, :]], axis=1)
        a_hi, a_lo = split(block_f)
        cols = slice(kt * 256, (kt + 1) * 256)
        reduced = reduced + dot3(a_hi, a_lo, bv_h[:, cols], bv_l[:, cols], NT)
    hi, lo = split(reduced.T)
    red_h[...] = hi
    red_l[...] = lo

    def rows_of(base, size):
        return pl.ds(pl.multiple_of(base, size), size)

    def copy(src_ref, dst_ref, send, recv, dev):
        return pltpu.make_async_remote_copy(
            src_ref=src_ref, dst_ref=dst_ref, send_sem=send, recv_sem=recv, device_id=dev, device_id_type=MESH
        )

    def cols_of(k):
        return slice(k * KC, (k + 1) * KC)

    def core_copy(k):
        return copy(
            part.at[rows_of((1 - core) * 128, 128), pl.ds(k * KC, KC)],
            core_in.at[k],
            core_send.at[k],
            core_recv.at[k],
            dom_id(peer),
        )

    def z1_copies(k):
        return (
            copy(
                core_sum.at[k, rows_of((1 - s1) * 32, 32), :],
                z1_in.at[k, 0],
                z1_send.at[k, 0],
                z1_recv.at[k, 0],
                dom_id(za),
            ),
            copy(
                core_sum.at[k, rows_of(64 + (1 - t1) * 32, 32), :],
                z1_in.at[k, 1],
                z1_send.at[k, 1],
                z1_recv.at[k, 1],
                dom_id(zb),
            ),
        )

    def z2_copies(k):
        return (
            copy(
                z1_sum.at[k, 0, rows_of((1 - s2) * 16, 16), :],
                z2_in.at[k, 0],
                z2_send.at[k, 0],
                z2_recv.at[k, 0],
                dom_id(zb),
            ),
            copy(
                z1_sum.at[k, 1, rows_of((1 - t2) * 16, 16), :],
                z2_in.at[k, 1],
                z2_send.at[k, 1],
                z2_recv.at[k, 1],
                dom_id(za),
            ),
        )

    row_1 = core * 128 + s1 * 32 + s2 * 16
    row_2 = core * 128 + 64 + t1 * 32 + t2 * 16

    def plane_copy(k, o):
        q = (p + o) % 16
        return copy(
            block.at[k, rows_of((q // 4) * 8, 8), pl.ds(pl.multiple_of((q % 4) * KQ, KQ), KQ)],
            plane_in.at[k, o],
            plane_send.at[k, o],
            plane_recv.at[k, o],
            plane_id(q),
        )

    my_tile = p // 4
    my_row = jnp.where(my_tile < 2, row_1 + my_tile * 8, row_2 + (my_tile - 2) * 8)
    del my_row
    half = my_tile // 2
    own_row = row_1 + half * (row_2 - row_1) + (my_tile % 2) * 8
    own_lane = (p % 4) * KQ

    def own_tile(k):
        return (rows_of(own_row, 8), pl.ds(pl.multiple_of(k * KC + own_lane, KQ), KQ))

    def back_copy(k, o):
        q = (p + o) % 16
        return copy(
            back_out.at[k, q // 2],
            upd.at[own_tile(k)],
            back_send.at[k, o],
            back_recv.at[k, o],
            plane_id(q),
        )

    def back_wait(k, o):
        q = (p + 16 - o) % 16
        tile = q // 4
        row = row_1 + (tile // 2) * (row_2 - row_1) + (tile % 2) * 8
        dst = upd.at[rows_of(row, 8), pl.ds(pl.multiple_of(k * KC + (q % 4) * KQ, KQ), KQ)]
        copy(back_out.at[k, 0], dst, back_send.at[k, o], back_recv.at[k, o], plane_id(q)).wait_recv()

    def g2_copies(k):
        a = upd.at[rows_of(row_1, 16), pl.ds(k * KC, KC)]
        b = upd.at[rows_of(row_2, 16), pl.ds(k * KC, KC)]
        return (
            copy(a, a, g2_send.at[k, 0], g2_recv.at[k, 0], dom_id(zb)),
            copy(b, b, g2_send.at[k, 1], g2_recv.at[k, 1], dom_id(za)),
        )

    def g2_waits(k):
        a = upd.at[rows_of(core * 128 + s1 * 32 + (1 - s2) * 16, 16), pl.ds(k * KC, KC)]
        b = upd.at[rows_of(core * 128 + 64 + t1 * 32 + (1 - t2) * 16, 16), pl.ds(k * KC, KC)]
        copy(a, a, g2_send.at[k, 0], g2_recv.at[k, 0], dom_id(zb)).wait_recv()
        copy(b, b, g2_send.at[k, 1], g2_recv.at[k, 1], dom_id(za)).wait_recv()

    def g1_copies(k):
        a = upd.at[rows_of(core * 128 + s1 * 32, 32), pl.ds(k * KC, KC)]
        b = upd.at[rows_of(core * 128 + 64 + t1 * 32, 32), pl.ds(k * KC, KC)]
        return (
            copy(a, a, g1_send.at[k, 0], g1_recv.at[k, 0], dom_id(za)),
            copy(b, b, g1_send.at[k, 1], g1_recv.at[k, 1], dom_id(zb)),
        )

    def g1_waits(k):
        a = upd.at[rows_of(core * 128 + (1 - s1) * 32, 32), pl.ds(k * KC, KC)]
        b = upd.at[rows_of(core * 128 + 64 + (1 - t1) * 32, 32), pl.ds(k * KC, KC)]
        copy(a, a, g1_send.at[k, 0], g1_recv.at[k, 0], dom_id(za)).wait_recv()
        copy(b, b, g1_send.at[k, 1], g1_recv.at[k, 1], dom_id(zb)).wait_recv()

    def gc_copy(k):
        a = upd.at[rows_of(core * 128, 128), pl.ds(k * KC, KC)]
        return copy(a, a, gc_send.at[k], gc_recv.at[k], dom_id(peer))

    def gc_wait(k):
        a = upd.at[rows_of((1 - core) * 128, 128), pl.ds(k * KC, KC)]
        copy(a, a, gc_send.at[k], gc_recv.at[k], dom_id(peer)).wait_recv()

    fac_x = power(lev_x)
    fac_v = power(lev_v)

    def stage_project(k):
        part[:, cols_of(k)] = dot3(red_h[...], red_l[...], bx_h[0:ROWS, cols_of(k)], bx_l[0:ROWS, cols_of(k)], NN)
        core_copy(k).start()

    def stage_core(k):
        core_copy(k).wait_recv()
        core_sum[k] = part[rows_of(core * 128, 128), cols_of(k)] + core_in[k]
        for cp in z1_copies(k):
            cp.start()

    def stage_z1(k):
        for cp in z1_copies(k):
            cp.wait_recv()
        z1_sum[k, 0] = core_sum[k, rows_of(s1 * 32, 32), :] + z1_in[k, 0]
        z1_sum[k, 1] = core_sum[k, rows_of(64 + t1 * 32, 32), :] + z1_in[k, 1]
        for cp in z2_copies(k):
            cp.start()

    def stage_z2(k):
        for cp in z2_copies(k):
            cp.wait_recv()
        for h, (keep, base) in enumerate(((s2, row_1), (t2, row_2))):
            total = z1_sum[k, h, rows_of(keep * 16, 16), :] + z2_in[k, h]
            mode_x = (lax.broadcasted_iota(jnp.int32, (16, KC), 1) + k * KC).astype(F32)
            mode_v = (lax.broadcasted_iota(jnp.int32, (16, KC), 0) + base).astype(F32)
            bend_x = mode_x * fac_x * (1.0 / MX)
            bend_v = mode_v * fac_v * (1.0 / MV)
            weight = 1.0 / ((1.0 + bend_x * bend_x) * (1.0 + bend_v * bend_v))
            scale_x = jnp.where(mode_x == 0.0, 1.0 / NX, 2.0 / NX).astype(F32)
            scale_v = jnp.where(mode_v == 0.0, 1.0 / NV, 2.0 / NV).astype(F32)
            block[k, h * 16 : (h + 1) * 16, :] = total * (weight * (scale_x * scale_v))
        for o in range(1, 16):
            plane_copy(k, o).start()

    def stage_plane(k):
        mine = block[k, rows_of((p // 4) * 8, 8), pl.ds(pl.multiple_of((p % 4) * KQ, KQ), KQ)]
        plane_in[k, 0] = mine
        for o in range(1, 16):
            plane_copy(k, o).wait_recv()
        if k == 0:
            for o in range(1, 8):
                copy(
                    coef_own, coef_all.at[(c + 8 - o) % 8], coef_send.at[o], coef_recv.at[o], {"comp": c, "dom": d}
                ).wait_recv()
        own = []
        for g in range(8):
            a = plane_in[k, (p + 16 - 2 * g) % 16]
            b = plane_in[k, (p + 16 - 2 * g - 1) % 16]
            own.append(a + b)
        total = jnp.zeros((8, KQ), F32)
        for g in range(8):
            total = total + coef_all[g][:, 0:1] * own[g]
        for g in range(8):
            back_out[k, g] = total - own[g]
        upd[own_tile(k)] = back_out[k, c]
        for o in range(1, 16):
            back_copy(k, o).start()

    def stage_back(k):
        for o in range(1, 16):
            back_wait(k, o)
        for cp in g2_copies(k):
            cp.start()

    def stage_g2(k):
        g2_waits(k)
        for cp in g1_copies(k):
            cp.start()

    def stage_g1(k):
        g1_waits(k)
        gc_copy(k).start()

    def stage_gc(k):
        gc_wait(k)
        u_hi, u_lo = split(upd[:, cols_of(k)])
        term = dot3(bx_h[:, cols_of(k)], bx_l[:, cols_of(k)], u_hi, u_lo, NT)
        if k == 0:
            corr[...] = term
        else:
            corr[...] += term

    stages = (stage_project, stage_core, stage_z1, stage_z2, stage_plane, stage_back, stage_g2, stage_g1, stage_gc)
    for tick in range(NCH + len(stages) - 1):
        for s in reversed(range(len(stages))):
            if 0 <= tick - s < NCH:
                stages[s](tick - s)

    c_hi, c_lo = split(corr[...])
    for kt in range(TILES // 2):
        cols = slice(kt * 256, (kt + 1) * 256)
        add = dot3(c_hi, c_lo, bv_h[:, cols], bv_l[:, cols], NN)
        for t in range(2):
            part_t = add[:, t * LANES : (t + 1) * LANES]
            fa[2 * kt + t, LEAD : LEAD + ROWS + 8, :] += part_t[0 : ROWS + 8]
            fa[2 * kt + t, LEAD - 8 : LEAD, :] += part_t[ROWS + 8 :]

    rate = set_rates(jnp.float32(1.0))
    step(fa, fb, LEAD - 8, WIDE, rate)

    def store(t, quarter):
        return pltpu.make_async_copy(
            fa.at[t, pl.ds(LEAD + quarter * 96, 96), :],
            out_ref.at[0, pl.ds(quarter * 96, 96), pl.ds(t * LANES, LANES)],
            out_sem.at[quarter, t],
        )

    for quarter in range(4):
        step(fb, fa, LEAD + quarter * 96, 96, rate)
        for t in range(TILES):
            store(t, quarter).start()

    for o in range(1, 8):
        coef_copy(o).wait_send()
    for k in range(NCH):
        core_copy(k).wait_send()
        gc_copy(k).wait_send()
        for group in (z1_copies(k), z2_copies(k), g2_copies(k), g1_copies(k)):
            for cp in group:
                cp.wait_send()
        for o in range(1, 16):
            plane_copy(k, o).wait_send()
            back_copy(k, o).wait_send()
    for quarter in range(4):
        for t in range(TILES):
            store(t, quarter).wait()


def body(densities, levels, coeffs):
    dma = pltpu.SemaphoreType.DMA
    vmem = pltpu.VMEM
    return pl.pallas_call(
        kernel,
        out_shape=jax.ShapeDtypeStruct((1, ROWS, NV), F32),
        in_specs=[
            pl.BlockSpec(memory_space=pltpu.SMEM),
            pl.BlockSpec(memory_space=pltpu.SMEM),
            pl.BlockSpec(memory_space=pl.ANY),
        ],
        out_specs=pl.BlockSpec(memory_space=pl.ANY),
        scratch_shapes=[
            vmem((TILES, PLANE_ROWS, LANES), F32),
            vmem((TILES, PLANE_ROWS, LANES), F32),
            vmem((TILES, 8, LANES), F32),
            vmem((TILES, 8, LANES), F32),
            vmem((WIDE, MX), BF16),
            vmem((WIDE, MX), BF16),
            vmem((MV, NV), BF16),
            vmem((MV, NV), BF16),
            vmem((MV, ROWS), BF16),
            vmem((MV, ROWS), BF16),
            vmem((MV, MX), F32),
            vmem((NCH, 128, KC), F32),
            vmem((NCH, 128, KC), F32),
            vmem((NCH, 2, 32, KC), F32),
            vmem((NCH, 2, 32, KC), F32),
            vmem((NCH, 2, 16, KC), F32),
            vmem((NCH, 32, KC), F32),
            vmem((NCH, 16, 8, KQ), F32),
            vmem((NCH, 8, 8, KQ), F32),
            vmem((MV, MX), F32),
            vmem((WIDE, MV), F32),
            vmem((8, LANES), F32),
            vmem((8, 8, LANES), F32),
            dma((TILES,)),
            dma((4, TILES)),
            dma((2,)),
            dma((2,)),
            dma((8,)),
            dma((8,)),
            dma((NCH,)),
            dma((NCH,)),
            dma((NCH, 2)),
            dma((NCH, 2)),
            dma((NCH, 2)),
            dma((NCH, 2)),
            dma((NCH, 16)),
            dma((NCH, 16)),
            dma((NCH, 16)),
            dma((NCH, 16)),
            dma((NCH, 2)),
            dma((NCH, 2)),
            dma((NCH, 2)),
            dma((NCH, 2)),
            dma((NCH,)),
            dma((NCH,)),
        ],
        compiler_params=pltpu.CompilerParams(
            collective_id=0, has_side_effects=True, vmem_limit_bytes=60 * 1024 * 1024
        ),
        name="window",
    )(levels, coeffs, densities)


def solution(mesh):
    placed = (P("comp", "dom", None), P("comp", None), P("comp"))
    return jax.shard_map(
        body, mesh=mesh, in_specs=placed, out_specs=P("comp", "dom", None), check_vma=False
    )
```

```python
import functools

import jax
import jax.numpy as jnp
import numpy as np
from jax import lax
from jax.experimental import pallas as pl
from jax.experimental.pallas import tpu as pltpu
from jax.sharding import PartitionSpec as P

MX = 2048
MV = 256
PRE = 8
POST = 2
NV = 2048
ROWS = 384
NX = 6144
LANES = 128
TILES = NV // LANES
HALO = 16
SPAN = 4
LEAD = 64
WIDE = SPAN * LANES
PAD = 8
BLOCKS = 8
NCH = 2
KC = MX // NCH
KQ = KC // 4
MESH = pl.DeviceIdType.MESH
F32 = jnp.float32
BF16 = jnp.bfloat16

TWO_PI_HI = float(np.float32(6.28125))
TWO_PI_LO = float(np.float32(2.0 * np.pi - 6.28125))
INV_TWO_PI = float(np.float32(1.0 / (2.0 * np.pi)))


def sine_terms():
    count = 6
    nodes = np.cos(np.pi * (np.arange(64) + 0.5) / 128)
    r = np.pi * nodes
    u = r * r
    basis = np.stack([u**i for i in range(count)], axis=1)
    target = np.sqrt(2.0) * np.sin(r / 2) / r
    terms, *_ = np.linalg.lstsq(basis * r[:, None], target * r, rcond=None)
    return [float(np.float32(t)) for t in terms]


SINE_TERMS = sine_terms()


def cosine(phase):
    turns = jnp.round(phase * INV_TWO_PI)
    r = (phase - turns * TWO_PI_HI) - turns * TWO_PI_LO
    u = r * r
    s = jnp.full_like(u, SINE_TERMS[-1])
    for term in SINE_TERMS[-2::-1]:
        s = s * u + term
    s = s * r
    return 1.0 - s * s


def split(x):
    hi = x.astype(BF16)
    return hi, (x - hi.astype(F32)).astype(BF16)


scope = jax.named_scope


def dot3(a_hi, a_lo, b_hi, b_lo, dims):
    def dot(a, b):
        return lax.dot_general(a, b, (dims, ((), ())), preferred_element_type=F32)

    return dot(a_hi, b_hi) + dot(a_hi, b_lo) + dot(a_lo, b_hi)


NN = ((1,), (0,))
NT = ((1,), (1,))


def kernel(
    lev_ref,
    coef_ref,
    dens_ref,
    out_ref,
    cells,
    fa,
    fb,
    bx_h,
    bx_l,
    bv_h,
    bv_l,
    bt_h,
    bt_l,
    red_h,
    red_l,
    part,
    core_in,
    core_sum,
    z1_in,
    z1_sum,
    z2_in,
    block,
    plane_in,
    back_out,
    upd,
    corr,
    coef_own,
    coef_all,
    in_sem,
    out_sem,
    halo_send,
    halo_recv,
    coef_send,
    coef_recv,
    core_send,
    core_recv,
    z1_send,
    z1_recv,
    z2_send,
    z2_recv,
    plane_send,
    plane_recv,
    back_send,
    back_recv,
    g2_send,
    g2_recv,
    g1_send,
    g1_recv,
    gc_send,
    gc_recv,
):
    c = lax.axis_index("comp")
    d = lax.axis_index("dom")
    z = d // 4
    xh = (d // 2) % 2
    core = d % 2
    p = c * 2 + xh
    nxt = (d + 1) % 16
    prv = (d + 15) % 16
    peer = d + 1 - 2 * core
    za = (z + 1 - 2 * (z % 2)) * 4 + d % 4
    zb = (3 - z) * 4 + d % 4
    s1 = (z % 2 + z // 2) % 2
    s2 = z // 2
    t1 = z // 2
    t2 = s1

    def dom_id(dom):
        return {"comp": c, "dom": dom}

    def plane_id(q):
        return {"comp": q // 2, "dom": z * 4 + (q % 2) * 2 + core}

    barrier = pltpu.get_barrier_semaphore()
    for dom in (nxt, prv, peer, za, zb):
        pl.semaphore_signal(barrier, inc=1, device_id=dom_id(dom), device_id_type=MESH)
    for o in range(1, 16):
        q = (p + o) % 16
        pl.semaphore_signal(barrier, inc=1, device_id=plane_id(q), device_id_type=MESH)

    def load(t):
        return pltpu.make_async_copy(
            dens_ref.at[0, :, pl.ds(t * LANES, LANES)],
            cells.at[t, pl.ds(LEAD, ROWS), :],
            in_sem.at[t],
        )

    for t in range(TILES):
        load(t).start()

    lev_x = lev_ref[0, 0]
    lev_v = lev_ref[0, 1]
    courant = 0.3 + lev_x.astype(F32) / 15.0
    diffusion = 0.1 + lev_v.astype(F32) / 30.0
    coef_own[...] = jnp.full((8, LANES), coef_ref[0].astype(F32), F32)
    coef_all[c] = coef_own[...]

    def power(level):
        return jnp.where(level == 0, 8.0, jnp.where(level == 1, 4.0, jnp.where(level == 2, 2.0, 1.0))).astype(F32)

    lane = lax.broadcasted_iota(jnp.int32, (16, LANES), 1)
    row16 = lax.broadcasted_iota(jnp.int32, (16, LANES), 0)

    def mode_rows(i, _):
        mode = (row16 + i * 16).astype(F32)
        r0 = pl.multiple_of(i * 16, 16)
        for t in range(TILES):
            cell = (lane + t * LANES).astype(F32)
            phase = ((np.float32(np.pi) * (cell + 0.5)) * mode) * np.float32(1.0 / NV)
            hi, lo = split(cosine(phase))
            bv_h[pl.ds(r0, 16), t * LANES : (t + 1) * LANES] = hi
            bv_l[pl.ds(r0, 16), t * LANES : (t + 1) * LANES] = lo
        return 0

    def cell_rows(i, _):
        for b in range(4):
            r0 = pl.multiple_of(i * 64 + b * 16, 16)
            angle = np.float32(np.pi) * ((row16 + r0).astype(F32) + 0.5)
            for t in range(MV // LANES):
                mode = (lane + t * LANES).astype(F32)
                phase = (angle * mode) * np.float32(1.0 / NV)
                hi, lo = split(cosine(phase))
                bt_h[pl.ds(r0, 16), t * LANES : (t + 1) * LANES] = hi
                bt_l[pl.ds(r0, 16), t * LANES : (t + 1) * LANES] = lo
        return 0

    def space_basis(k, i):
        local = (row16 + (i % 8) * 16) * SPAN + i // 8 - LEAD
        cell = local + d * ROWS
        cell = jnp.where(cell < 0, cell + NX, cell)
        cell = jnp.where(cell >= NX, cell - NX, cell)
        angle = np.float32(np.pi) * (cell.astype(F32) + 0.5)
        r0 = pl.multiple_of(i * 16, 16)
        for t in range(k * KC // LANES, (k + 1) * KC // LANES):
            mode = (lane + t * LANES).astype(F32)
            phase = (angle * mode) * np.float32(1.0 / NX)
            hi, lo = split(cosine(phase))
            bx_h[pl.ds(r0, 16), t * LANES : (t + 1) * LANES] = hi
            bx_l[pl.ds(r0, 16), t * LANES : (t + 1) * LANES] = lo

    def fill_space_basis(k):
        def run(i, _):
            space_basis(k, 2 * i)
            space_basis(k, 2 * i + 1)
            return 0

        lax.fori_loop(0, WIDE // 32, run, 0)

    with scope("A_bv"):
        lax.fori_loop(0, MV // 16, mode_rows, 0)
        fill_space_basis(0)

    with scope('B_barrier'):
        for t in range(TILES):
            load(t).wait()
        pl.semaphore_wait(barrier, 20)

    halo_up = pltpu.make_async_remote_copy(
        src_ref=cells.at[pl.ds(0, 9), pl.ds(LEAD, HALO), :],
        dst_ref=cells.at[pl.ds(0, 9), pl.ds(LEAD + ROWS, HALO), :],
        send_sem=halo_send.at[0],
        recv_sem=halo_recv.at[0],
        device_id=dom_id(prv),
        device_id_type=MESH,
    )
    halo_down = pltpu.make_async_remote_copy(
        src_ref=cells.at[pl.ds(7, 9), pl.ds(LEAD + ROWS - HALO, HALO), :],
        dst_ref=cells.at[pl.ds(7, 9), pl.ds(LEAD - HALO, HALO), :],
        send_sem=halo_send.at[1],
        recv_sem=halo_recv.at[1],
        device_id=dom_id(nxt),
        device_id_type=MESH,
    )
    halo_up.start()
    halo_down.start()

    def coef_copy(o):
        return pltpu.make_async_remote_copy(
            src_ref=coef_own,
            dst_ref=coef_all.at[c],
            send_sem=coef_send.at[o],
            recv_sem=coef_recv.at[o],
            device_id={"comp": (c + o) % 8, "dom": d},
            device_id_type=MESH,
        )

    for o in range(1, 8):
        coef_copy(o).start()

    with scope("C_bx"):
        for k in range(1, NCH):
            fill_space_basis(k)

    def edges(dst):
        for q in range(SPAN):
            dst[q, PAD - 1 : PAD, :] = dst[q, PAD : PAD + 1, :]
            dst[q, PAD + NV : PAD + NV + 1, :] = dst[q, PAD + NV - 1 : PAD + NV, :]

    row_v = lax.broadcasted_iota(jnp.int32, (16, LANES), 0)
    offsets = (2.0 * row_v.astype(F32) + 1.0) / NV - 1.0

    def step(src, dst, active, scale, unit):
        rate = active * diffusion
        share = (1.0 / diffusion) if unit else scale
        keep = (1.0 - 2.0 * rate) * share
        pace = active * courant * share
        side = rate * share
        size = 16 * BLOCKS

        def rows(upper):
            base = NV // 2 if upper else 0
            edge = SPAN - 1 if upper else 0
            count = NV // 2 // size

            def turned(i):
                r0 = pl.multiple_of(i * size + base + PAD, 8)
                return tuple(
                    pltpu.roll(src[edge, pl.ds(r0 + b * 16, 16), :], 1 if upper else LANES - 1, 1)
                    for b in range(BLOCKS)
                )

            def run(i, ends):
                ahead = turned((i + 1) % count)
                for b in range(BLOCKS):
                    first = i * size + (base + b * 16)
                    r = pl.multiple_of(first + PAD, 8)
                    velocity = offsets + first.astype(F32) * (2.0 / NV)
                    be = velocity * (pace if upper else -pace)
                    al = keep - be
                    f = [src[q, pl.ds(r, 16), :] for q in range(SPAN)]
                    shifted = [ends[b]] + f[:-1] if upper else f[1:] + [ends[b]]
                    for q in range(SPAN):
                        pair = src[q, pl.ds(r - 1, 16), :] + src[q, pl.ds(r + 1, 16), :]
                        if not unit:
                            pair = side * pair
                        dst[q, pl.ds(r, 16), :] = al * f[q] + be * shifted[q] + pair
                return ahead

            lax.fori_loop(0, count, run, turned(0))

        rows(False)
        rows(True)
        edges(dst)

    with scope('D_halo'):
        halo_up.wait_recv()
        halo_down.wait_recv()
        halo_up.wait_send()
        halo_down.wait_send()
    with scope("E_turn"):

        def turn_in(t, _):
            for q in range(SPAN):
                tile = cells[t, pl.ds(q, LANES, stride=SPAN), :]
                fa[q, pl.ds(pl.multiple_of(PAD + t * LANES, 8), LANES), :] = tile.T
            return 0

        lax.fori_loop(0, TILES, turn_in, 0, unroll=4)
        edges(fa)
    src, dst = fa, fb
    scale = diffusion * diffusion
    scale = scale * scale * diffusion
    for s in range(PRE):
        with scope("E_step"):
            if s < PRE - 3:
                step(src, dst, 1.0, 1.0, True)
            else:
                active = jnp.where(lev_x > s - (PRE - 3), 1.0, 0.0).astype(F32)
                step(src, dst, active, scale if s == PRE - 3 else 1.0, False)
        src, dst = dst, src

    with scope("F_reduced"):
        own_lanes = lax.broadcasted_iota(jnp.int32, (MV, 2 * LANES), 1) % LANES
        own_lanes = (own_lanes >= LEAD // SPAN) & (own_lanes < (LEAD + ROWS) // SPAN)
        for half in range(2):
            reduced = jnp.zeros((MV, 2 * LANES), F32)
            for kt in range(TILES // 2):
                cut = slice(PAD + kt * 256, PAD + (kt + 1) * 256)
                cols = slice(kt * 256, (kt + 1) * 256)
                f = jnp.concatenate([fa[2 * half, cut, :], fa[2 * half + 1, cut, :]], axis=1)
                f_hi, f_lo = split(f)
                reduced = reduced + dot3(bv_h[:, cols], bv_l[:, cols], f_hi, f_lo, NN)
            hi, lo = split(jnp.where(own_lanes, reduced, 0.0))
            red_h[:, half * 256 : (half + 1) * 256] = hi
            red_l[:, half * 256 : (half + 1) * 256] = lo

    def rows_of(base, size):
        return pl.ds(pl.multiple_of(base, size), size)

    def copy(src_ref, dst_ref, send, recv, dev):
        return pltpu.make_async_remote_copy(
            src_ref=src_ref, dst_ref=dst_ref, send_sem=send, recv_sem=recv, device_id=dev, device_id_type=MESH
        )

    def cols_of(k):
        return slice(k * KC, (k + 1) * KC)

    def core_copy(k):
        return copy(
            part.at[rows_of((1 - core) * 128, 128), pl.ds(k * KC, KC)],
            core_in.at[k],
            core_send.at[k],
            core_recv.at[k],
            dom_id(peer),
        )

    def z1_copies(k):
        return (
            copy(
                core_sum.at[k, rows_of((1 - s1) * 32, 32), :],
                z1_in.at[k, 0],
                z1_send.at[k, 0],
                z1_recv.at[k, 0],
                dom_id(za),
            ),
            copy(
                core_sum.at[k, rows_of(64 + (1 - t1) * 32, 32), :],
                z1_in.at[k, 1],
                z1_send.at[k, 1],
                z1_recv.at[k, 1],
                dom_id(zb),
            ),
        )

    def z2_copies(k):
        return (
            copy(
                z1_sum.at[k, 0, rows_of((1 - s2) * 16, 16), :],
                z2_in.at[k, 0],
                z2_send.at[k, 0],
                z2_recv.at[k, 0],
                dom_id(zb),
            ),
            copy(
                z1_sum.at[k, 1, rows_of((1 - t2) * 16, 16), :],
                z2_in.at[k, 1],
                z2_send.at[k, 1],
                z2_recv.at[k, 1],
                dom_id(za),
            ),
        )

    row_1 = core * 128 + s1 * 32 + s2 * 16
    row_2 = core * 128 + 64 + t1 * 32 + t2 * 16

    def plane_copy(k, o):
        q = (p + o) % 16
        return copy(
            block.at[k, rows_of((q // 4) * 8, 8), pl.ds(pl.multiple_of((q % 4) * KQ, KQ), KQ)],
            plane_in.at[k, o],
            plane_send.at[k, o],
            plane_recv.at[k, o],
            plane_id(q),
        )

    my_tile = p // 4
    half = my_tile // 2
    own_row = row_1 + half * (row_2 - row_1) + (my_tile % 2) * 8
    own_lane = (p % 4) * KQ

    def own_tile(k):
        return (rows_of(own_row, 8), pl.ds(pl.multiple_of(k * KC + own_lane, KQ), KQ))

    def back_copy(k, o):
        q = (p + o) % 16
        return copy(
            back_out.at[k, q // 2],
            upd.at[own_tile(k)],
            back_send.at[k, o],
            back_recv.at[k, o],
            plane_id(q),
        )

    def back_wait(k, o):
        q = (p + 16 - o) % 16
        tile = q // 4
        row = row_1 + (tile // 2) * (row_2 - row_1) + (tile % 2) * 8
        dst = upd.at[rows_of(row, 8), pl.ds(pl.multiple_of(k * KC + (q % 4) * KQ, KQ), KQ)]
        copy(back_out.at[k, 0], dst, back_send.at[k, o], back_recv.at[k, o], plane_id(q)).wait_recv()

    def g2_copies(k):
        a = upd.at[rows_of(row_1, 16), pl.ds(k * KC, KC)]
        b = upd.at[rows_of(row_2, 16), pl.ds(k * KC, KC)]
        return (
            copy(a, a, g2_send.at[k, 0], g2_recv.at[k, 0], dom_id(zb)),
            copy(b, b, g2_send.at[k, 1], g2_recv.at[k, 1], dom_id(za)),
        )

    def g2_waits(k):
        a = upd.at[rows_of(core * 128 + s1 * 32 + (1 - s2) * 16, 16), pl.ds(k * KC, KC)]
        b = upd.at[rows_of(core * 128 + 64 + t1 * 32 + (1 - t2) * 16, 16), pl.ds(k * KC, KC)]
        copy(a, a, g2_send.at[k, 0], g2_recv.at[k, 0], dom_id(zb)).wait_recv()
        copy(b, b, g2_send.at[k, 1], g2_recv.at[k, 1], dom_id(za)).wait_recv()

    def g1_copies(k):
        a = upd.at[rows_of(core * 128 + s1 * 32, 32), pl.ds(k * KC, KC)]
        b = upd.at[rows_of(core * 128 + 64 + t1 * 32, 32), pl.ds(k * KC, KC)]
        return (
            copy(a, a, g1_send.at[k, 0], g1_recv.at[k, 0], dom_id(za)),
            copy(b, b, g1_send.at[k, 1], g1_recv.at[k, 1], dom_id(zb)),
        )

    def g1_waits(k):
        a = upd.at[rows_of(core * 128 + (1 - s1) * 32, 32), pl.ds(k * KC, KC)]
        b = upd.at[rows_of(core * 128 + 64 + (1 - t1) * 32, 32), pl.ds(k * KC, KC)]
        copy(a, a, g1_send.at[k, 0], g1_recv.at[k, 0], dom_id(za)).wait_recv()
        copy(b, b, g1_send.at[k, 1], g1_recv.at[k, 1], dom_id(zb)).wait_recv()

    def gc_copy(k):
        a = upd.at[rows_of(core * 128, 128), pl.ds(k * KC, KC)]
        return copy(a, a, gc_send.at[k], gc_recv.at[k], dom_id(peer))

    def gc_wait(k):
        a = upd.at[rows_of((1 - core) * 128, 128), pl.ds(k * KC, KC)]
        copy(a, a, gc_send.at[k], gc_recv.at[k], dom_id(peer)).wait_recv()

    fac_x = power(lev_x)
    fac_v = power(lev_v)

    def stage_project(k):
        part[:, cols_of(k)] = dot3(red_h[...], red_l[...], bx_h[:, cols_of(k)], bx_l[:, cols_of(k)], NN)
        core_copy(k).start()

    def stage_core(k):
        core_copy(k).wait_recv()
        core_sum[k] = part[rows_of(core * 128, 128), cols_of(k)] + core_in[k]
        for cp in z1_copies(k):
            cp.start()

    def stage_z1(k):
        for cp in z1_copies(k):
            cp.wait_recv()
        z1_sum[k, 0] = core_sum[k, rows_of(s1 * 32, 32), :] + z1_in[k, 0]
        z1_sum[k, 1] = core_sum[k, rows_of(64 + t1 * 32, 32), :] + z1_in[k, 1]
        for cp in z2_copies(k):
            cp.start()

    def stage_z2(k):
        for cp in z2_copies(k):
            cp.wait_recv()
        for h, (keep, base) in enumerate(((s2, row_1), (t2, row_2))):
            total = z1_sum[k, h, rows_of(keep * 16, 16), :] + z2_in[k, h]
            mode_x = (lax.broadcasted_iota(jnp.int32, (16, KC), 1) + k * KC).astype(F32)
            mode_v = (lax.broadcasted_iota(jnp.int32, (16, KC), 0) + base).astype(F32)
            bend_x = mode_x * fac_x * (1.0 / MX)
            bend_v = mode_v * fac_v * (1.0 / MV)
            weight = 1.0 / ((1.0 + bend_x * bend_x) * (1.0 + bend_v * bend_v))
            scale_x = jnp.where(mode_x == 0.0, 1.0 / NX, 2.0 / NX).astype(F32)
            scale_v = jnp.where(mode_v == 0.0, 1.0 / NV, 2.0 / NV).astype(F32)
            block[k, h * 16 : (h + 1) * 16, :] = total * (weight * (scale_x * scale_v))
        for o in range(1, 16):
            plane_copy(k, o).start()

    def stage_plane(k):
        mine = block[k, rows_of((p // 4) * 8, 8), pl.ds(pl.multiple_of((p % 4) * KQ, KQ), KQ)]
        plane_in[k, 0] = mine
        for o in range(1, 16):
            plane_copy(k, o).wait_recv()
        if k == 0:
            for o in range(1, 8):
                copy(
                    coef_own, coef_all.at[(c + 8 - o) % 8], coef_send.at[o], coef_recv.at[o], {"comp": c, "dom": d}
                ).wait_recv()
        own = []
        for g in range(8):
            a = plane_in[k, (p + 16 - 2 * g) % 16]
            b = plane_in[k, (p + 16 - 2 * g - 1) % 16]
            own.append(a + b)
        total = jnp.zeros((8, KQ), F32)
        for g in range(8):
            total = total + coef_all[g][:, 0:1] * own[g]
        for g in range(8):
            back_out[k, g] = total - own[g]
        upd[own_tile(k)] = back_out[k, c]
        for o in range(1, 16):
            back_copy(k, o).start()

    def stage_back(k):
        for o in range(1, 16):
            back_wait(k, o)
        for cp in g2_copies(k):
            cp.start()

    def stage_g2(k):
        g2_waits(k)
        for cp in g1_copies(k):
            cp.start()

    def stage_g1(k):
        g1_waits(k)
        gc_copy(k).start()

    def stage_gc(k):
        gc_wait(k)
        u_hi, u_lo = split(upd[:, cols_of(k)])
        term = dot3(u_hi, u_lo, bx_h[:, cols_of(k)], bx_l[:, cols_of(k)], NT)
        if k == 0:
            corr[...] = term
        else:
            corr[...] += term

    stages = (stage_project, stage_core, stage_z1, stage_z2, stage_plane, stage_back, stage_g2, stage_g1, stage_gc)
    for tick in range(NCH + len(stages) - 1):
        for s in reversed(range(len(stages))):
            if 0 <= tick - s < NCH:
                with scope('G_%d_%s' % (tick - s, stages[s].__name__)):
                    stages[s](tick - s)
        if tick == 1:
            with scope("G_bt"):
                lax.fori_loop(0, NV // 64, cell_rows, 0)

    with scope("H_expand"):
        for half in range(2):
            c_hi, c_lo = split(corr[:, half * 256 : (half + 1) * 256])
            for kt in range(TILES // 2):
                rows = slice(kt * 256, (kt + 1) * 256)
                cut = slice(PAD + kt * 256, PAD + (kt + 1) * 256)
                add = dot3(bt_h[rows, :], bt_l[rows, :], c_hi, c_lo, NN)
                fa[2 * half, cut, :] += add[:, :LANES]
                fa[2 * half + 1, cut, :] += add[:, LANES:]
        edges(fa)

    with scope("I_post"):
        step(fa, fb, 1.0, 1.0, True)
        step(fb, fa, 1.0, diffusion, False)

    def store(t):
        return pltpu.make_async_copy(
            cells.at[t, pl.ds(LEAD, ROWS), :],
            out_ref.at[0, :, pl.ds(pl.multiple_of(t * LANES, LANES), LANES)],
            out_sem.at[t],
        )

    with scope("J_turn"):
        low, high = LEAD // SPAN, (LEAD + ROWS) // SPAN

        def turn_out(t, _):
            for q in range(SPAN):
                tile = fa[q, pl.ds(pl.multiple_of(PAD + t * LANES, 8), LANES), :].T
                cells[t, pl.ds(LEAD + q, high - low, stride=SPAN), :] = tile[low:high]
            store(t).start()
            return 0

        lax.fori_loop(0, TILES, turn_out, 0, unroll=4)

    with scope('K_tail'):
        for o in range(1, 8):
            coef_copy(o).wait_send()
        for k in range(NCH):
            core_copy(k).wait_send()
            gc_copy(k).wait_send()
            for group in (z1_copies(k), z2_copies(k), g2_copies(k), g1_copies(k)):
                for cp in group:
                    cp.wait_send()
            for o in range(1, 16):
                plane_copy(k, o).wait_send()
                back_copy(k, o).wait_send()
        for t in range(TILES):
            store(t).wait()


def body(densities, levels, coeffs):
    dma = pltpu.SemaphoreType.DMA
    vmem = pltpu.VMEM
    return pl.pallas_call(
        kernel,
        out_shape=jax.ShapeDtypeStruct((1, ROWS, NV), F32),
        in_specs=[
            pl.BlockSpec(memory_space=pltpu.SMEM),
            pl.BlockSpec(memory_space=pltpu.SMEM),
            pl.BlockSpec(memory_space=pl.ANY),
        ],
        out_specs=pl.BlockSpec(memory_space=pl.ANY),
        scratch_shapes=[
            vmem((TILES, WIDE, LANES), F32),
            vmem((SPAN, NV + 2 * PAD, LANES), F32),
            vmem((SPAN, NV + 2 * PAD, LANES), F32),
            vmem((WIDE, MX), BF16),
            vmem((WIDE, MX), BF16),
            vmem((MV, NV), BF16),
            vmem((MV, NV), BF16),
            vmem((NV, MV), BF16),
            vmem((NV, MV), BF16),
            vmem((MV, WIDE), BF16),
            vmem((MV, WIDE), BF16),
            vmem((MV, MX), F32),
            vmem((NCH, 128, KC), F32),
            vmem((NCH, 128, KC), F32),
            vmem((NCH, 2, 32, KC), F32),
            vmem((NCH, 2, 32, KC), F32),
            vmem((NCH, 2, 16, KC), F32),
            vmem((NCH, 32, KC), F32),
            vmem((NCH, 16, 8, KQ), F32),
            vmem((NCH, 8, 8, KQ), F32),
            vmem((MV, MX), F32),
            vmem((MV, WIDE), F32),
            vmem((8, LANES), F32),
            vmem((8, 8, LANES), F32),
            dma((TILES,)),
            dma((TILES,)),
            dma((2,)),
            dma((2,)),
            dma((8,)),
            dma((8,)),
            dma((NCH,)),
            dma((NCH,)),
            dma((NCH, 2)),
            dma((NCH, 2)),
            dma((NCH, 2)),
            dma((NCH, 2)),
            dma((NCH, 16)),
            dma((NCH, 16)),
            dma((NCH, 16)),
            dma((NCH, 16)),
            dma((NCH, 2)),
            dma((NCH, 2)),
            dma((NCH, 2)),
            dma((NCH, 2)),
            dma((NCH,)),
            dma((NCH,)),
        ],
        compiler_params=pltpu.CompilerParams(
            collective_id=0, has_side_effects=True, vmem_limit_bytes=60 * 1024 * 1024
        ),
        name="window",
    )(levels, coeffs, densities)


def solution(mesh):
    placed = (P("comp", "dom", None), P("comp", None), P("comp"))
    return jax.shard_map(
        body, mesh=mesh, in_specs=placed, out_specs=P("comp", "dom", None), check_vma=False
    )
```

```python
import functools

import jax
import jax.numpy as jnp
import numpy as np
from jax import lax
from jax.experimental import pallas as pl
from jax.experimental.pallas import tpu as pltpu
from jax.sharding import PartitionSpec as P

MX = 2048
MV = 256
PRE = 8
POST = 2
NV = 2048
ROWS = 384
NX = 6144
LANES = 128
TILES = NV // LANES
HALO = 16
SPAN = 4
LEAD = 64
WIDE = SPAN * LANES
PAD = 8
NCH = 2
KC = MX // NCH
KQ = KC // 4
MESH = pl.DeviceIdType.MESH
F32 = jnp.float32
BF16 = jnp.bfloat16

TWO_PI_HI = float(np.float32(6.28125))
TWO_PI_LO = float(np.float32(2.0 * np.pi - 6.28125))
INV_TWO_PI = float(np.float32(1.0 / (2.0 * np.pi)))


def sine_terms():
    count = 6
    nodes = np.cos(np.pi * (np.arange(64) + 0.5) / 128)
    r = np.pi * nodes
    u = r * r
    basis = np.stack([u**i for i in range(count)], axis=1)
    target = np.sqrt(2.0) * np.sin(r / 2) / r
    terms, *_ = np.linalg.lstsq(basis * r[:, None], target * r, rcond=None)
    return [float(np.float32(t)) for t in terms]


SINE_TERMS = sine_terms()


def cosine(phase):
    turns = jnp.round(phase * INV_TWO_PI)
    r = (phase - turns * TWO_PI_HI) - turns * TWO_PI_LO
    u = r * r
    s = jnp.full_like(u, SINE_TERMS[-1])
    for term in SINE_TERMS[-2::-1]:
        s = s * u + term
    s = s * r
    return 1.0 - s * s


def split(x):
    hi = x.astype(BF16)
    return hi, (x - hi.astype(F32)).astype(BF16)


scope = jax.named_scope


def dot3(a_hi, a_lo, b_hi, b_lo, dims):
    def dot(a, b):
        return lax.dot_general(a, b, (dims, ((), ())), preferred_element_type=F32)

    return dot(a_hi, b_hi) + dot(a_hi, b_lo) + dot(a_lo, b_hi)


NN = ((1,), (0,))
NT = ((1,), (1,))


def kernel(
    lev_ref,
    coef_ref,
    dens_ref,
    out_ref,
    cells,
    fa,
    fb,
    bx_h,
    bx_l,
    bv_h,
    bv_l,
    bt_h,
    bt_l,
    red_h,
    red_l,
    part,
    core_in,
    core_sum,
    z1_in,
    z1_sum,
    z2_in,
    block,
    plane_in,
    back_out,
    upd,
    corr,
    coef_own,
    coef_all,
    in_sem,
    out_sem,
    halo_send,
    halo_recv,
    coef_send,
    coef_recv,
    core_send,
    core_recv,
    z1_send,
    z1_recv,
    z2_send,
    z2_recv,
    plane_send,
    plane_recv,
    back_send,
    back_recv,
    g2_send,
    g2_recv,
    g1_send,
    g1_recv,
    gc_send,
    gc_recv,
):
    c = lax.axis_index("comp")
    d = lax.axis_index("dom")
    z = d // 4
    xh = (d // 2) % 2
    core = d % 2
    p = c * 2 + xh
    nxt = (d + 1) % 16
    prv = (d + 15) % 16
    peer = d + 1 - 2 * core
    za = (z + 1 - 2 * (z % 2)) * 4 + d % 4
    zb = (3 - z) * 4 + d % 4
    s1 = (z % 2 + z // 2) % 2
    s2 = z // 2
    t1 = z // 2
    t2 = s1

    def dom_id(dom):
        return {"comp": c, "dom": dom}

    def plane_id(q):
        return {"comp": q // 2, "dom": z * 4 + (q % 2) * 2 + core}

    barrier = pltpu.get_barrier_semaphore()
    for dom in (nxt, prv, peer, za, zb):
        pl.semaphore_signal(barrier, inc=1, device_id=dom_id(dom), device_id_type=MESH)
    for o in range(1, 16):
        q = (p + o) % 16
        pl.semaphore_signal(barrier, inc=1, device_id=plane_id(q), device_id_type=MESH)

    def load(t):
        return pltpu.make_async_copy(
            dens_ref.at[0, :, pl.ds(t * LANES, LANES)],
            cells.at[t, pl.ds(LEAD, ROWS), :],
            in_sem.at[t],
        )

    for t in range(TILES):
        load(t).start()

    lev_x = lev_ref[0, 0]
    lev_v = lev_ref[0, 1]
    courant = 0.3 + lev_x.astype(F32) / 15.0
    diffusion = 0.1 + lev_v.astype(F32) / 30.0
    coef_own[...] = jnp.full((8, LANES), coef_ref[0].astype(F32), F32)
    coef_all[c] = coef_own[...]

    def power(level):
        return jnp.where(level == 0, 8.0, jnp.where(level == 1, 4.0, jnp.where(level == 2, 2.0, 1.0))).astype(F32)

    lane = lax.broadcasted_iota(jnp.int32, (16, LANES), 1)
    row16 = lax.broadcasted_iota(jnp.int32, (16, LANES), 0)

    def mode_rows(i, _):
        mode = (row16 + i * 16).astype(F32)
        r0 = pl.multiple_of(i * 16, 16)
        for t in range(TILES):
            cell = (lane + t * LANES).astype(F32)
            phase = ((np.float32(np.pi) * (cell + 0.5)) * mode) * np.float32(1.0 / NV)
            hi, lo = split(cosine(phase))
            bv_h[pl.ds(r0, 16), t * LANES : (t + 1) * LANES] = hi
            bv_l[pl.ds(r0, 16), t * LANES : (t + 1) * LANES] = lo
        return 0

    def cell_rows(i, _):
        for b in range(4):
            r0 = pl.multiple_of(i * 64 + b * 16, 16)
            angle = np.float32(np.pi) * ((row16 + r0).astype(F32) + 0.5)
            for t in range(MV // LANES):
                mode = (lane + t * LANES).astype(F32)
                phase = (angle * mode) * np.float32(1.0 / NV)
                hi, lo = split(cosine(phase))
                bt_h[pl.ds(r0, 16), t * LANES : (t + 1) * LANES] = hi
                bt_l[pl.ds(r0, 16), t * LANES : (t + 1) * LANES] = lo
        return 0

    def space_basis(k, i):
        local = (row16 + (i % 8) * 16) * SPAN + i // 8 - LEAD
        cell = local + d * ROWS
        cell = jnp.where(cell < 0, cell + NX, cell)
        cell = jnp.where(cell >= NX, cell - NX, cell)
        angle = np.float32(np.pi) * (cell.astype(F32) + 0.5)
        r0 = pl.multiple_of(i * 16, 16)
        for t in range(k * KC // LANES, (k + 1) * KC // LANES):
            mode = (lane + t * LANES).astype(F32)
            phase = (angle * mode) * np.float32(1.0 / NX)
            hi, lo = split(cosine(phase))
            bx_h[pl.ds(r0, 16), t * LANES : (t + 1) * LANES] = hi
            bx_l[pl.ds(r0, 16), t * LANES : (t + 1) * LANES] = lo

    def fill_space_basis(k):
        def run(i, _):
            space_basis(k, 2 * i)
            space_basis(k, 2 * i + 1)
            return 0

        lax.fori_loop(0, WIDE // 32, run, 0)

    with scope("A_bv"):
        lax.fori_loop(0, MV // 16, mode_rows, 0)
        fill_space_basis(0)

    with scope('B_barrier'):
        for t in range(TILES):
            load(t).wait()
        pl.semaphore_wait(barrier, 20)

    halo_up = pltpu.make_async_remote_copy(
        src_ref=cells.at[pl.ds(0, 9), pl.ds(LEAD, HALO), :],
        dst_ref=cells.at[pl.ds(0, 9), pl.ds(LEAD + ROWS, HALO), :],
        send_sem=halo_send.at[0],
        recv_sem=halo_recv.at[0],
        device_id=dom_id(prv),
        device_id_type=MESH,
    )
    halo_down = pltpu.make_async_remote_copy(
        src_ref=cells.at[pl.ds(7, 9), pl.ds(LEAD + ROWS - HALO, HALO), :],
        dst_ref=cells.at[pl.ds(7, 9), pl.ds(LEAD - HALO, HALO), :],
        send_sem=halo_send.at[1],
        recv_sem=halo_recv.at[1],
        device_id=dom_id(nxt),
        device_id_type=MESH,
    )
    halo_up.start()
    halo_down.start()

    def coef_copy(o):
        return pltpu.make_async_remote_copy(
            src_ref=coef_own,
            dst_ref=coef_all.at[c],
            send_sem=coef_send.at[o],
            recv_sem=coef_recv.at[o],
            device_id={"comp": (c + o) % 8, "dom": d},
            device_id_type=MESH,
        )

    for o in range(1, 8):
        coef_copy(o).start()

    with scope("C_bx"):
        for k in range(1, NCH):
            fill_space_basis(k)

    def edges(dst):
        for q in range(SPAN):
            dst[q, PAD - 1 : PAD, :] = dst[q, PAD : PAD + 1, :]
            dst[q, PAD + NV : PAD + NV + 1, :] = dst[q, PAD + NV - 1 : PAD + NV, :]

    row_v = lax.broadcasted_iota(jnp.int32, (16, LANES), 0)
    offsets = (2.0 * row_v.astype(F32) + 1.0) / NV - 1.0

    def step(src, dst, active):
        rate = active * diffusion
        keep = 1.0 - 2.0 * rate
        pace = active * courant

        def part_of(first, upper):
            r = first + PAD
            velocity = offsets + first * (2.0 / NV)
            be = velocity * (pace if upper else -pace)
            al = keep - be
            f = [src[q, r : r + 16, :] for q in range(SPAN)]
            if upper:
                shifted = [pltpu.roll(f[SPAN - 1], 1, 1)] + f[:-1]
            else:
                shifted = f[1:] + [pltpu.roll(f[0], LANES - 1, 1)]
            for q in range(SPAN):
                pair = src[q, r - 1 : r + 15, :] + src[q, r + 1 : r + 17, :]
                dst[q, r : r + 16, :] = al * f[q] + be * shifted[q] + rate * pair

        for first in range(0, NV, 16):
            part_of(first, first >= NV // 2)
        edges(dst)

    with scope('D_halo'):
        halo_up.wait_recv()
        halo_down.wait_recv()
        halo_up.wait_send()
        halo_down.wait_send()
    with scope("E_turn"):

        def turn_in(t, _):
            for q in range(SPAN):
                tile = cells[t, pl.ds(q, LANES, stride=SPAN), :]
                fa[q, pl.ds(pl.multiple_of(PAD + t * LANES, 8), LANES), :] = tile.T
            return 0

        lax.fori_loop(0, TILES, turn_in, 0, unroll=4)
        edges(fa)
    def correct():
        with scope("F_reduced"):
            own_lanes = lax.broadcasted_iota(jnp.int32, (MV, 2 * LANES), 1) % LANES
            own_lanes = (own_lanes >= LEAD // SPAN) & (own_lanes < (LEAD + ROWS) // SPAN)
            for half in range(2):
                reduced = jnp.zeros((MV, 2 * LANES), F32)
                for kt in range(TILES // 2):
                    cut = slice(PAD + kt * 256, PAD + (kt + 1) * 256)
                    cols = slice(kt * 256, (kt + 1) * 256)
                    f = jnp.concatenate([fa[2 * half, cut, :], fa[2 * half + 1, cut, :]], axis=1)
                    f_hi, f_lo = split(f)
                    reduced = reduced + dot3(bv_h[:, cols], bv_l[:, cols], f_hi, f_lo, NN)
                hi, lo = split(jnp.where(own_lanes, reduced, 0.0))
                red_h[:, half * 256 : (half + 1) * 256] = hi
                red_l[:, half * 256 : (half + 1) * 256] = lo

        def rows_of(base, size):
            return pl.ds(pl.multiple_of(base, size), size)

        def copy(src_ref, dst_ref, send, recv, dev):
            return pltpu.make_async_remote_copy(
                src_ref=src_ref, dst_ref=dst_ref, send_sem=send, recv_sem=recv, device_id=dev, device_id_type=MESH
            )

        def cols_of(k):
            return slice(k * KC, (k + 1) * KC)

        def core_copy(k):
            return copy(
                part.at[rows_of((1 - core) * 128, 128), pl.ds(k * KC, KC)],
                core_in.at[k],
                core_send.at[k],
                core_recv.at[k],
                dom_id(peer),
            )

        def z1_copies(k):
            return (
                copy(
                    core_sum.at[k, rows_of((1 - s1) * 32, 32), :],
                    z1_in.at[k, 0],
                    z1_send.at[k, 0],
                    z1_recv.at[k, 0],
                    dom_id(za),
                ),
                copy(
                    core_sum.at[k, rows_of(64 + (1 - t1) * 32, 32), :],
                    z1_in.at[k, 1],
                    z1_send.at[k, 1],
                    z1_recv.at[k, 1],
                    dom_id(zb),
                ),
            )

        def z2_copies(k):
            return (
                copy(
                    z1_sum.at[k, 0, rows_of((1 - s2) * 16, 16), :],
                    z2_in.at[k, 0],
                    z2_send.at[k, 0],
                    z2_recv.at[k, 0],
                    dom_id(zb),
                ),
                copy(
                    z1_sum.at[k, 1, rows_of((1 - t2) * 16, 16), :],
                    z2_in.at[k, 1],
                    z2_send.at[k, 1],
                    z2_recv.at[k, 1],
                    dom_id(za),
                ),
            )

        row_1 = core * 128 + s1 * 32 + s2 * 16
        row_2 = core * 128 + 64 + t1 * 32 + t2 * 16

        def plane_copy(k, o):
            q = (p + o) % 16
            return copy(
                block.at[k, rows_of((q // 4) * 8, 8), pl.ds(pl.multiple_of((q % 4) * KQ, KQ), KQ)],
                plane_in.at[k, o],
                plane_send.at[k, o],
                plane_recv.at[k, o],
                plane_id(q),
            )

        my_tile = p // 4
        half = my_tile // 2
        own_row = row_1 + half * (row_2 - row_1) + (my_tile % 2) * 8
        own_lane = (p % 4) * KQ

        def own_tile(k):
            return (rows_of(own_row, 8), pl.ds(pl.multiple_of(k * KC + own_lane, KQ), KQ))

        def back_copy(k, o):
            q = (p + o) % 16
            return copy(
                back_out.at[k, q // 2],
                upd.at[own_tile(k)],
                back_send.at[k, o],
                back_recv.at[k, o],
                plane_id(q),
            )

        def back_wait(k, o):
            q = (p + 16 - o) % 16
            tile = q // 4
            row = row_1 + (tile // 2) * (row_2 - row_1) + (tile % 2) * 8
            dst = upd.at[rows_of(row, 8), pl.ds(pl.multiple_of(k * KC + (q % 4) * KQ, KQ), KQ)]
            copy(back_out.at[k, 0], dst, back_send.at[k, o], back_recv.at[k, o], plane_id(q)).wait_recv()

        def g2_copies(k):
            a = upd.at[rows_of(row_1, 16), pl.ds(k * KC, KC)]
            b = upd.at[rows_of(row_2, 16), pl.ds(k * KC, KC)]
            return (
                copy(a, a, g2_send.at[k, 0], g2_recv.at[k, 0], dom_id(zb)),
                copy(b, b, g2_send.at[k, 1], g2_recv.at[k, 1], dom_id(za)),
            )

        def g2_waits(k):
            a = upd.at[rows_of(core * 128 + s1 * 32 + (1 - s2) * 16, 16), pl.ds(k * KC, KC)]
            b = upd.at[rows_of(core * 128 + 64 + t1 * 32 + (1 - t2) * 16, 16), pl.ds(k * KC, KC)]
            copy(a, a, g2_send.at[k, 0], g2_recv.at[k, 0], dom_id(zb)).wait_recv()
            copy(b, b, g2_send.at[k, 1], g2_recv.at[k, 1], dom_id(za)).wait_recv()

        def g1_copies(k):
            a = upd.at[rows_of(core * 128 + s1 * 32, 32), pl.ds(k * KC, KC)]
            b = upd.at[rows_of(core * 128 + 64 + t1 * 32, 32), pl.ds(k * KC, KC)]
            return (
                copy(a, a, g1_send.at[k, 0], g1_recv.at[k, 0], dom_id(za)),
                copy(b, b, g1_send.at[k, 1], g1_recv.at[k, 1], dom_id(zb)),
            )

        def g1_waits(k):
            a = upd.at[rows_of(core * 128 + (1 - s1) * 32, 32), pl.ds(k * KC, KC)]
            b = upd.at[rows_of(core * 128 + 64 + (1 - t1) * 32, 32), pl.ds(k * KC, KC)]
            copy(a, a, g1_send.at[k, 0], g1_recv.at[k, 0], dom_id(za)).wait_recv()
            copy(b, b, g1_send.at[k, 1], g1_recv.at[k, 1], dom_id(zb)).wait_recv()

        def gc_copy(k):
            a = upd.at[rows_of(core * 128, 128), pl.ds(k * KC, KC)]
            return copy(a, a, gc_send.at[k], gc_recv.at[k], dom_id(peer))

        def gc_wait(k):
            a = upd.at[rows_of((1 - core) * 128, 128), pl.ds(k * KC, KC)]
            copy(a, a, gc_send.at[k], gc_recv.at[k], dom_id(peer)).wait_recv()

        fac_x = power(lev_x)
        fac_v = power(lev_v)

        def stage_project(k):
            part[:, cols_of(k)] = dot3(red_h[...], red_l[...], bx_h[:, cols_of(k)], bx_l[:, cols_of(k)], NN)
            core_copy(k).start()

        def stage_core(k):
            core_copy(k).wait_recv()
            core_sum[k] = part[rows_of(core * 128, 128), cols_of(k)] + core_in[k]
            for cp in z1_copies(k):
                cp.start()

        def stage_z1(k):
            for cp in z1_copies(k):
                cp.wait_recv()
            z1_sum[k, 0] = core_sum[k, rows_of(s1 * 32, 32), :] + z1_in[k, 0]
            z1_sum[k, 1] = core_sum[k, rows_of(64 + t1 * 32, 32), :] + z1_in[k, 1]
            for cp in z2_copies(k):
                cp.start()

        def stage_z2(k):
            for cp in z2_copies(k):
                cp.wait_recv()
            for h, (keep, base) in enumerate(((s2, row_1), (t2, row_2))):
                total = z1_sum[k, h, rows_of(keep * 16, 16), :] + z2_in[k, h]
                mode_x = (lax.broadcasted_iota(jnp.int32, (16, KC), 1) + k * KC).astype(F32)
                mode_v = (lax.broadcasted_iota(jnp.int32, (16, KC), 0) + base).astype(F32)
                bend_x = mode_x * fac_x * (1.0 / MX)
                bend_v = mode_v * fac_v * (1.0 / MV)
                weight = 1.0 / ((1.0 + bend_x * bend_x) * (1.0 + bend_v * bend_v))
                scale_x = jnp.where(mode_x == 0.0, 1.0 / NX, 2.0 / NX).astype(F32)
                scale_v = jnp.where(mode_v == 0.0, 1.0 / NV, 2.0 / NV).astype(F32)
                block[k, h * 16 : (h + 1) * 16, :] = total * (weight * (scale_x * scale_v))
            for o in range(1, 16):
                plane_copy(k, o).start()

        def stage_plane(k):
            mine = block[k, rows_of((p // 4) * 8, 8), pl.ds(pl.multiple_of((p % 4) * KQ, KQ), KQ)]
            plane_in[k, 0] = mine
            for o in range(1, 16):
                plane_copy(k, o).wait_recv()
            if k == 0:
                for o in range(1, 8):
                    copy(
                        coef_own, coef_all.at[(c + 8 - o) % 8], coef_send.at[o], coef_recv.at[o], {"comp": c, "dom": d}
                    ).wait_recv()
            own = []
            for g in range(8):
                a = plane_in[k, (p + 16 - 2 * g) % 16]
                b = plane_in[k, (p + 16 - 2 * g - 1) % 16]
                own.append(a + b)
            total = jnp.zeros((8, KQ), F32)
            for g in range(8):
                total = total + coef_all[g][:, 0:1] * own[g]
            for g in range(8):
                back_out[k, g] = total - own[g]
            upd[own_tile(k)] = back_out[k, c]
            for o in range(1, 16):
                back_copy(k, o).start()

        def stage_back(k):
            for o in range(1, 16):
                back_wait(k, o)
            for cp in g2_copies(k):
                cp.start()

        def stage_g2(k):
            g2_waits(k)
            for cp in g1_copies(k):
                cp.start()

        def stage_g1(k):
            g1_waits(k)
            gc_copy(k).start()

        def stage_gc(k):
            gc_wait(k)
            u_hi, u_lo = split(upd[:, cols_of(k)])
            term = dot3(u_hi, u_lo, bx_h[:, cols_of(k)], bx_l[:, cols_of(k)], NT)
            if k == 0:
                corr[...] = term
            else:
                corr[...] += term

        stages = (stage_project, stage_core, stage_z1, stage_z2, stage_plane, stage_back, stage_g2, stage_g1, stage_gc)
        for tick in range(NCH + len(stages) - 1):
            for s in reversed(range(len(stages))):
                if 0 <= tick - s < NCH:
                    with scope('G_%d_%s' % (tick - s, stages[s].__name__)):
                        stages[s](tick - s)
            if tick == 1:
                with scope("G_bt"):
                    lax.fori_loop(0, NV // 64, cell_rows, 0)

        with scope("H_expand"):
            for half in range(2):
                c_hi, c_lo = split(corr[:, half * 256 : (half + 1) * 256])
                for kt in range(TILES // 2):
                    rows = slice(kt * 256, (kt + 1) * 256)
                    cut = slice(PAD + kt * 256, PAD + (kt + 1) * 256)
                    add = dot3(bt_h[rows, :], bt_l[rows, :], c_hi, c_lo, NN)
                    fa[2 * half, cut, :] += add[:, :LANES]
                    fa[2 * half + 1, cut, :] += add[:, LANES:]
            edges(fa)

        with scope('H_sent'):
            for o in range(1, 8):
                coef_copy(o).wait_send()
            for k in range(NCH):
                core_copy(k).wait_send()
                gc_copy(k).wait_send()
                for group in (z1_copies(k), z2_copies(k), g2_copies(k), g1_copies(k)):
                    for cp in group:
                        cp.wait_send()
                for o in range(1, 16):
                    plane_copy(k, o).wait_send()
                    back_copy(k, o).wait_send()


    def two_steps(i, _):
        @pl.when(i == PRE // 2)
        def _():
            correct()

        with scope("E_step"):
            for src, dst, s in ((fa, fb, 2 * i), (fb, fa, 2 * i + 1)):
                on = (lev_x + (PRE - 3) > s) | (s >= PRE)
                step(src, dst, jnp.where(on, 1.0, 0.0).astype(F32))
        return 0

    lax.fori_loop(0, (PRE + POST) // 2, two_steps, 0)

    def store(t):
        return pltpu.make_async_copy(
            cells.at[t, pl.ds(LEAD, ROWS), :],
            out_ref.at[0, :, pl.ds(pl.multiple_of(t * LANES, LANES), LANES)],
            out_sem.at[t],
        )

    with scope("J_turn"):
        low, high = LEAD // SPAN, (LEAD + ROWS) // SPAN

        def turn_out(t, _):
            for q in range(SPAN):
                tile = fa[q, pl.ds(pl.multiple_of(PAD + t * LANES, 8), LANES), :].T
                cells[t, pl.ds(LEAD + q, high - low, stride=SPAN), :] = tile[low:high]
            store(t).start()
            return 0

        lax.fori_loop(0, TILES, turn_out, 0, unroll=4)

    with scope('K_tail'):
        for t in range(TILES):
            store(t).wait()


def body(densities, levels, coeffs):
    dma = pltpu.SemaphoreType.DMA
    vmem = pltpu.VMEM
    return pl.pallas_call(
        kernel,
        out_shape=jax.ShapeDtypeStruct((1, ROWS, NV), F32),
        in_specs=[
            pl.BlockSpec(memory_space=pltpu.SMEM),
            pl.BlockSpec(memory_space=pltpu.SMEM),
            pl.BlockSpec(memory_space=pl.ANY),
        ],
        out_specs=pl.BlockSpec(memory_space=pl.ANY),
        scratch_shapes=[
            vmem((TILES, WIDE, LANES), F32),
            vmem((SPAN, NV + 2 * PAD, LANES), F32),
            vmem((SPAN, NV + 2 * PAD, LANES), F32),
            vmem((WIDE, MX), BF16),
            vmem((WIDE, MX), BF16),
            vmem((MV, NV), BF16),
            vmem((MV, NV), BF16),
            vmem((NV, MV), BF16),
            vmem((NV, MV), BF16),
            vmem((MV, WIDE), BF16),
            vmem((MV, WIDE), BF16),
            vmem((MV, MX), F32),
            vmem((NCH, 128, KC), F32),
            vmem((NCH, 128, KC), F32),
            vmem((NCH, 2, 32, KC), F32),
            vmem((NCH, 2, 32, KC), F32),
            vmem((NCH, 2, 16, KC), F32),
            vmem((NCH, 32, KC), F32),
            vmem((NCH, 16, 8, KQ), F32),
            vmem((NCH, 8, 8, KQ), F32),
            vmem((MV, MX), F32),
            vmem((MV, WIDE), F32),
            vmem((8, LANES), F32),
            vmem((8, 8, LANES), F32),
            dma((TILES,)),
            dma((TILES,)),
            dma((2,)),
            dma((2,)),
            dma((8,)),
            dma((8,)),
            dma((NCH,)),
            dma((NCH,)),
            dma((NCH, 2)),
            dma((NCH, 2)),
            dma((NCH, 2)),
            dma((NCH, 2)),
            dma((NCH, 16)),
            dma((NCH, 16)),
            dma((NCH, 16)),
            dma((NCH, 16)),
            dma((NCH, 2)),
            dma((NCH, 2)),
            dma((NCH, 2)),
            dma((NCH, 2)),
            dma((NCH,)),
            dma((NCH,)),
        ],
        compiler_params=pltpu.CompilerParams(
            collective_id=0, has_side_effects=True, vmem_limit_bytes=60 * 1024 * 1024
        ),
        name="window",
    )(levels, coeffs, densities)


def solution(mesh):
    placed = (P("comp", "dom", None), P("comp", None), P("comp"))
    return jax.shard_map(
        body, mesh=mesh, in_specs=placed, out_specs=P("comp", "dom", None), check_vma=False
    )
```

```python
import functools

import jax
import jax.numpy as jnp
import numpy as np
from jax import lax
from jax.experimental import pallas as pl
from jax.experimental.pallas import tpu as pltpu
from jax.sharding import PartitionSpec as P

MX = 2048
MV = 256
PRE = 8
POST = 2
NV = 2048
ROWS = 384
NX = 6144
LANES = 128
TILES = NV // LANES
HALO = 16
SPAN = 4
LEAD = 64
WIDE = SPAN * LANES
PAD = 8
EARLY = 3
NCH = 4
KC = MX // NCH
KQ = KC // 4
MESH = pl.DeviceIdType.MESH
F32 = jnp.float32
BF16 = jnp.bfloat16

TWO_PI_HI = float(np.float32(6.28125))
TWO_PI_LO = float(np.float32(2.0 * np.pi - 6.28125))
INV_TWO_PI = float(np.float32(1.0 / (2.0 * np.pi)))


def sine_terms():
    count = 6
    nodes = np.cos(np.pi * (np.arange(64) + 0.5) / 128)
    r = np.pi * nodes
    u = r * r
    basis = np.stack([u**i for i in range(count)], axis=1)
    target = np.sqrt(2.0) * np.sin(r / 2) / r
    terms, *_ = np.linalg.lstsq(basis * r[:, None], target * r, rcond=None)
    return [float(np.float32(t)) for t in terms]


SINE_TERMS = sine_terms()


def cosine(phase):
    turns = jnp.round(phase * INV_TWO_PI)
    r = (phase - turns * TWO_PI_HI) - turns * TWO_PI_LO
    u = r * r
    s = jnp.full_like(u, SINE_TERMS[-1])
    for term in SINE_TERMS[-2::-1]:
        s = s * u + term
    s = s * r
    return 1.0 - s * s


def split(x):
    hi = x.astype(BF16)
    return hi, (x - hi.astype(F32)).astype(BF16)


scope = jax.named_scope


def dot3(a_hi, a_lo, b_hi, b_lo, dims):
    def dot(a, b):
        return lax.dot_general(a, b, (dims, ((), ())), preferred_element_type=F32)

    return dot(a_hi, b_hi) + dot(a_hi, b_lo) + dot(a_lo, b_hi)


NN = ((1,), (0,))
NT = ((1,), (1,))


def kernel(
    lev_ref,
    coef_ref,
    dens_ref,
    out_ref,
    cells,
    fa,
    fb,
    bx_h,
    bx_l,
    bv_h,
    bv_l,
    bt_h,
    bt_l,
    red_h,
    red_l,
    part,
    core_in,
    core_sum,
    z1_in,
    z1_sum,
    z2_in,
    block,
    plane_in,
    back_out,
    upd,
    corr,
    coef_own,
    coef_all,
    in_sem,
    out_sem,
    halo_send,
    halo_recv,
    coef_send,
    coef_recv,
    core_send,
    core_recv,
    z1_send,
    z1_recv,
    z2_send,
    z2_recv,
    plane_send,
    plane_recv,
    back_send,
    back_recv,
    g2_send,
    g2_recv,
    g1_send,
    g1_recv,
    gc_send,
    gc_recv,
):
    c = lax.axis_index("comp")
    d = lax.axis_index("dom")
    z = d // 4
    xh = (d // 2) % 2
    core = d % 2
    p = c * 2 + xh
    nxt = (d + 1) % 16
    prv = (d + 15) % 16
    peer = d + 1 - 2 * core
    za = (z + 1 - 2 * (z % 2)) * 4 + d % 4
    zb = (3 - z) * 4 + d % 4
    s1 = (z % 2 + z // 2) % 2
    s2 = z // 2
    t1 = z // 2
    t2 = s1

    def dom_id(dom):
        return {"comp": c, "dom": dom}

    def plane_id(q):
        return {"comp": q // 2, "dom": z * 4 + (q % 2) * 2 + core}

    barrier = pltpu.get_barrier_semaphore()
    for dom in (nxt, prv, peer, za, zb):
        pl.semaphore_signal(barrier, inc=1, device_id=dom_id(dom), device_id_type=MESH)
    for o in range(1, 16):
        q = (p + o) % 16
        pl.semaphore_signal(barrier, inc=1, device_id=plane_id(q), device_id_type=MESH)

    def load(t):
        return pltpu.make_async_copy(
            dens_ref.at[0, :, pl.ds(t * LANES, LANES)],
            cells.at[t, pl.ds(LEAD, ROWS), :],
            in_sem.at[t],
        )

    for t in range(TILES):
        load(t).start()

    lev_x = lev_ref[0, 0]
    lev_v = lev_ref[0, 1]
    courant = 0.3 + lev_x.astype(F32) / 15.0
    diffusion = 0.1 + lev_v.astype(F32) / 30.0
    coef_own[...] = jnp.full((8, LANES), coef_ref[0].astype(F32), F32)
    coef_all[c] = coef_own[...]

    def power(level):
        return jnp.where(level == 0, 8.0, jnp.where(level == 1, 4.0, jnp.where(level == 2, 2.0, 1.0))).astype(F32)

    lane = lax.broadcasted_iota(jnp.int32, (16, LANES), 1)
    row16 = lax.broadcasted_iota(jnp.int32, (16, LANES), 0)

    def mode_rows(i, _):
        mode = (row16 + i * 16).astype(F32)
        r0 = pl.multiple_of(i * 16, 16)
        for t in range(TILES):
            cell = (lane + t * LANES).astype(F32)
            phase = ((np.float32(np.pi) * (cell + 0.5)) * mode) * np.float32(1.0 / NV)
            hi, lo = split(cosine(phase))
            bv_h[pl.ds(r0, 16), t * LANES : (t + 1) * LANES] = hi
            bv_l[pl.ds(r0, 16), t * LANES : (t + 1) * LANES] = lo
        return 0

    def cell_rows(i, _):
        for b in range(4):
            r0 = pl.multiple_of(i * 64 + b * 16, 16)
            angle = np.float32(np.pi) * ((row16 + r0).astype(F32) + 0.5)
            for t in range(MV // LANES):
                mode = (lane + t * LANES).astype(F32)
                phase = (angle * mode) * np.float32(1.0 / NV)
                hi, lo = split(cosine(phase))
                bt_h[pl.ds(r0, 16), t * LANES : (t + 1) * LANES] = hi
                bt_l[pl.ds(r0, 16), t * LANES : (t + 1) * LANES] = lo
        return 0

    def space_basis(k, i):
        local = (row16 + (i % 8) * 16) * SPAN + i // 8 - LEAD
        cell = local + d * ROWS
        cell = jnp.where(cell < 0, cell + NX, cell)
        cell = jnp.where(cell >= NX, cell - NX, cell)
        angle = np.float32(np.pi) * (cell.astype(F32) + 0.5)
        r0 = pl.multiple_of(i * 16, 16)
        for t in range(k * KC // LANES, (k + 1) * KC // LANES):
            mode = (lane + t * LANES).astype(F32)
            phase = (angle * mode) * np.float32(1.0 / NX)
            hi, lo = split(cosine(phase))
            bx_h[pl.ds(r0, 16), t * LANES : (t + 1) * LANES] = hi
            bx_l[pl.ds(r0, 16), t * LANES : (t + 1) * LANES] = lo

    def fill_space_basis(k):
        def run(i, _):
            space_basis(k, 2 * i)
            space_basis(k, 2 * i + 1)
            return 0

        lax.fori_loop(0, WIDE // 32, run, 0)

    with scope("A_bv"):
        lax.fori_loop(0, MV // 16, mode_rows, 0)

    with scope('B_barrier'):
        for t in range(TILES):
            load(t).wait()
        pl.semaphore_wait(barrier, 20)

    halo_up = pltpu.make_async_remote_copy(
        src_ref=cells.at[pl.ds(0, 9), pl.ds(LEAD, HALO), :],
        dst_ref=cells.at[pl.ds(0, 9), pl.ds(LEAD + ROWS, HALO), :],
        send_sem=halo_send.at[0],
        recv_sem=halo_recv.at[0],
        device_id=dom_id(prv),
        device_id_type=MESH,
    )
    halo_down = pltpu.make_async_remote_copy(
        src_ref=cells.at[pl.ds(7, 9), pl.ds(LEAD + ROWS - HALO, HALO), :],
        dst_ref=cells.at[pl.ds(7, 9), pl.ds(LEAD - HALO, HALO), :],
        send_sem=halo_send.at[1],
        recv_sem=halo_recv.at[1],
        device_id=dom_id(nxt),
        device_id_type=MESH,
    )
    halo_up.start()
    halo_down.start()

    def coef_copy(o):
        return pltpu.make_async_remote_copy(
            src_ref=coef_own,
            dst_ref=coef_all.at[c],
            send_sem=coef_send.at[o],
            recv_sem=coef_recv.at[o],
            device_id={"comp": (c + o) % 8, "dom": d},
            device_id_type=MESH,
        )

    for o in range(1, 8):
        coef_copy(o).start()

    with scope("C_bx"):
        for k in range(EARLY):
            fill_space_basis(k)

    def edges(dst):
        for q in range(SPAN):
            dst[q, PAD - 1 : PAD, :] = dst[q, PAD : PAD + 1, :]
            dst[q, PAD + NV : PAD + NV + 1, :] = dst[q, PAD + NV - 1 : PAD + NV, :]

    row_v = lax.broadcasted_iota(jnp.int32, (16, LANES), 0)
    offsets = (2.0 * row_v.astype(F32) + 1.0) / NV - 1.0

    def step(src, dst, active):
        rate = active * diffusion
        keep = 1.0 - 2.0 * rate
        pace = active * courant

        def part_of(first, upper):
            r = first + PAD
            velocity = offsets + first * (2.0 / NV)
            be = velocity * (pace if upper else -pace)
            al = keep - be
            f = [src[q, r : r + 16, :] for q in range(SPAN)]
            if upper:
                shifted = [pltpu.roll(f[SPAN - 1], 1, 1)] + f[:-1]
            else:
                shifted = f[1:] + [pltpu.roll(f[0], LANES - 1, 1)]
            for q in range(SPAN):
                pair = src[q, r - 1 : r + 15, :] + src[q, r + 1 : r + 17, :]
                dst[q, r : r + 16, :] = al * f[q] + be * shifted[q] + rate * pair

        for first in range(0, NV, 16):
            part_of(first, first >= NV // 2)
        edges(dst)

    with scope('D_halo'):
        halo_up.wait_recv()
        halo_down.wait_recv()
        halo_up.wait_send()
        halo_down.wait_send()
    with scope("E_turn"):

        def turn_in(t, _):
            for q in range(SPAN):
                tile = cells[t, pl.ds(q, LANES, stride=SPAN), :]
                fa[q, pl.ds(pl.multiple_of(PAD + t * LANES, 8), LANES), :] = tile.T
            return 0

        lax.fori_loop(0, TILES, turn_in, 0, unroll=4)
        edges(fa)
    def correct():
        with scope("F_reduced"):
            own_lanes = lax.broadcasted_iota(jnp.int32, (MV, 2 * LANES), 1) % LANES
            own_lanes = (own_lanes >= LEAD // SPAN) & (own_lanes < (LEAD + ROWS) // SPAN)
            for half in range(2):
                reduced = jnp.zeros((MV, 2 * LANES), F32)
                for kt in range(TILES // 2):
                    cut = slice(PAD + kt * 256, PAD + (kt + 1) * 256)
                    cols = slice(kt * 256, (kt + 1) * 256)
                    f = jnp.concatenate([fa[2 * half, cut, :], fa[2 * half + 1, cut, :]], axis=1)
                    f_hi, f_lo = split(f)
                    reduced = reduced + dot3(bv_h[:, cols], bv_l[:, cols], f_hi, f_lo, NN)
                hi, lo = split(jnp.where(own_lanes, reduced, 0.0))
                red_h[:, half * 256 : (half + 1) * 256] = hi
                red_l[:, half * 256 : (half + 1) * 256] = lo

        def rows_of(base, size):
            return pl.ds(pl.multiple_of(base, size), size)

        def copy(src_ref, dst_ref, send, recv, dev):
            return pltpu.make_async_remote_copy(
                src_ref=src_ref, dst_ref=dst_ref, send_sem=send, recv_sem=recv, device_id=dev, device_id_type=MESH
            )

        def cols_of(k):
            return slice(k * KC, (k + 1) * KC)

        def core_copy(k):
            return copy(
                part.at[rows_of((1 - core) * 128, 128), pl.ds(k * KC, KC)],
                core_in.at[k],
                core_send.at[k],
                core_recv.at[k],
                dom_id(peer),
            )

        def z1_copies(k):
            return (
                copy(
                    core_sum.at[k, rows_of((1 - s1) * 32, 32), :],
                    z1_in.at[k, 0],
                    z1_send.at[k, 0],
                    z1_recv.at[k, 0],
                    dom_id(za),
                ),
                copy(
                    core_sum.at[k, rows_of(64 + (1 - t1) * 32, 32), :],
                    z1_in.at[k, 1],
                    z1_send.at[k, 1],
                    z1_recv.at[k, 1],
                    dom_id(zb),
                ),
            )

        def z2_copies(k):
            return (
                copy(
                    z1_sum.at[k, 0, rows_of((1 - s2) * 16, 16), :],
                    z2_in.at[k, 0],
                    z2_send.at[k, 0],
                    z2_recv.at[k, 0],
                    dom_id(zb),
                ),
                copy(
                    z1_sum.at[k, 1, rows_of((1 - t2) * 16, 16), :],
                    z2_in.at[k, 1],
                    z2_send.at[k, 1],
                    z2_recv.at[k, 1],
                    dom_id(za),
                ),
            )

        row_1 = core * 128 + s1 * 32 + s2 * 16
        row_2 = core * 128 + 64 + t1 * 32 + t2 * 16

        def plane_copy(k, o):
            q = (p + o) % 16
            return copy(
                block.at[k, rows_of((q // 4) * 8, 8), pl.ds(pl.multiple_of((q % 4) * KQ, KQ), KQ)],
                plane_in.at[k, o],
                plane_send.at[k, o],
                plane_recv.at[k, o],
                plane_id(q),
            )

        my_tile = p // 4
        half = my_tile // 2
        own_row = row_1 + half * (row_2 - row_1) + (my_tile % 2) * 8
        own_lane = (p % 4) * KQ

        def own_tile(k):
            return (rows_of(own_row, 8), pl.ds(pl.multiple_of(k * KC + own_lane, KQ), KQ))

        def back_copy(k, o):
            q = (p + o) % 16
            return copy(
                back_out.at[k, q // 2],
                upd.at[own_tile(k)],
                back_send.at[k, o],
                back_recv.at[k, o],
                plane_id(q),
            )

        def back_wait(k, o):
            q = (p + 16 - o) % 16
            tile = q // 4
            row = row_1 + (tile // 2) * (row_2 - row_1) + (tile % 2) * 8
            dst = upd.at[rows_of(row, 8), pl.ds(pl.multiple_of(k * KC + (q % 4) * KQ, KQ), KQ)]
            copy(back_out.at[k, 0], dst, back_send.at[k, o], back_recv.at[k, o], plane_id(q)).wait_recv()

        def g2_copies(k):
            a = upd.at[rows_of(row_1, 16), pl.ds(k * KC, KC)]
            b = upd.at[rows_of(row_2, 16), pl.ds(k * KC, KC)]
            return (
                copy(a, a, g2_send.at[k, 0], g2_recv.at[k, 0], dom_id(zb)),
                copy(b, b, g2_send.at[k, 1], g2_recv.at[k, 1], dom_id(za)),
            )

        def g2_waits(k):
            a = upd.at[rows_of(core * 128 + s1 * 32 + (1 - s2) * 16, 16), pl.ds(k * KC, KC)]
            b = upd.at[rows_of(core * 128 + 64 + t1 * 32 + (1 - t2) * 16, 16), pl.ds(k * KC, KC)]
            copy(a, a, g2_send.at[k, 0], g2_recv.at[k, 0], dom_id(zb)).wait_recv()
            copy(b, b, g2_send.at[k, 1], g2_recv.at[k, 1], dom_id(za)).wait_recv()

        def g1_copies(k):
            a = upd.at[rows_of(core * 128 + s1 * 32, 32), pl.ds(k * KC, KC)]
            b = upd.at[rows_of(core * 128 + 64 + t1 * 32, 32), pl.ds(k * KC, KC)]
            return (
                copy(a, a, g1_send.at[k, 0], g1_recv.at[k, 0], dom_id(za)),
                copy(b, b, g1_send.at[k, 1], g1_recv.at[k, 1], dom_id(zb)),
            )

        def g1_waits(k):
            a = upd.at[rows_of(core * 128 + (1 - s1) * 32, 32), pl.ds(k * KC, KC)]
            b = upd.at[rows_of(core * 128 + 64 + (1 - t1) * 32, 32), pl.ds(k * KC, KC)]
            copy(a, a, g1_send.at[k, 0], g1_recv.at[k, 0], dom_id(za)).wait_recv()
            copy(b, b, g1_send.at[k, 1], g1_recv.at[k, 1], dom_id(zb)).wait_recv()

        def gc_copy(k):
            a = upd.at[rows_of(core * 128, 128), pl.ds(k * KC, KC)]
            return copy(a, a, gc_send.at[k], gc_recv.at[k], dom_id(peer))

        def gc_wait(k):
            a = upd.at[rows_of((1 - core) * 128, 128), pl.ds(k * KC, KC)]
            copy(a, a, gc_send.at[k], gc_recv.at[k], dom_id(peer)).wait_recv()

        fac_x = power(lev_x)
        fac_v = power(lev_v)

        def stage_project(k):
            part[:, cols_of(k)] = dot3(red_h[...], red_l[...], bx_h[:, cols_of(k)], bx_l[:, cols_of(k)], NN)
            core_copy(k).start()

        def stage_core(k):
            core_copy(k).wait_recv()
            core_sum[k] = part[rows_of(core * 128, 128), cols_of(k)] + core_in[k]
            for cp in z1_copies(k):
                cp.start()

        def stage_z1(k):
            for cp in z1_copies(k):
                cp.wait_recv()
            z1_sum[k, 0] = core_sum[k, rows_of(s1 * 32, 32), :] + z1_in[k, 0]
            z1_sum[k, 1] = core_sum[k, rows_of(64 + t1 * 32, 32), :] + z1_in[k, 1]
            for cp in z2_copies(k):
                cp.start()

        def stage_z2(k):
            for cp in z2_copies(k):
                cp.wait_recv()
            for h, (keep, base) in enumerate(((s2, row_1), (t2, row_2))):
                total = z1_sum[k, h, rows_of(keep * 16, 16), :] + z2_in[k, h]
                mode_x = (lax.broadcasted_iota(jnp.int32, (16, KC), 1) + k * KC).astype(F32)
                mode_v = (lax.broadcasted_iota(jnp.int32, (16, KC), 0) + base).astype(F32)
                bend_x = mode_x * fac_x * (1.0 / MX)
                bend_v = mode_v * fac_v * (1.0 / MV)
                weight = 1.0 / ((1.0 + bend_x * bend_x) * (1.0 + bend_v * bend_v))
                scale_x = jnp.where(mode_x == 0.0, 1.0 / NX, 2.0 / NX).astype(F32)
                scale_v = jnp.where(mode_v == 0.0, 1.0 / NV, 2.0 / NV).astype(F32)
                block[k, h * 16 : (h + 1) * 16, :] = total * (weight * (scale_x * scale_v))
            for o in range(1, 16):
                plane_copy(k, o).start()

        def stage_plane(k):
            mine = block[k, rows_of((p // 4) * 8, 8), pl.ds(pl.multiple_of((p % 4) * KQ, KQ), KQ)]
            plane_in[k, 0] = mine
            for o in range(1, 16):
                plane_copy(k, o).wait_recv()
            if k == 0:
                for o in range(1, 8):
                    copy(
                        coef_own, coef_all.at[(c + 8 - o) % 8], coef_send.at[o], coef_recv.at[o], {"comp": c, "dom": d}
                    ).wait_recv()
            own = []
            for g in range(8):
                a = plane_in[k, (p + 16 - 2 * g) % 16]
                b = plane_in[k, (p + 16 - 2 * g - 1) % 16]
                own.append(a + b)
            total = jnp.zeros((8, KQ), F32)
            for g in range(8):
                total = total + coef_all[g][:, 0:1] * own[g]
            for g in range(8):
                back_out[k, g] = total - own[g]
            upd[own_tile(k)] = back_out[k, c]
            for o in range(1, 16):
                back_copy(k, o).start()

        def stage_back(k):
            for o in range(1, 16):
                back_wait(k, o)
            for cp in g2_copies(k):
                cp.start()

        def stage_g2(k):
            g2_waits(k)
            for cp in g1_copies(k):
                cp.start()

        def stage_g1(k):
            g1_waits(k)
            gc_copy(k).start()

        def stage_gc(k):
            gc_wait(k)
            u_hi, u_lo = split(upd[:, cols_of(k)])
            term = dot3(u_hi, u_lo, bx_h[:, cols_of(k)], bx_l[:, cols_of(k)], NT)
            if k == 0:
                corr[...] = term
            else:
                corr[...] += term

        stages = (stage_project, stage_core, stage_z1, stage_z2, stage_plane, stage_back, stage_g2, stage_g1, stage_gc)
        def run_stage(n, k):
            with scope("G_%d_%s" % (k, stages[n].__name__)):
                stages[n](k)

        for k in range(NCH):
            if k >= EARLY:
                fill_space_basis(k)
            run_stage(0, k)
            if k > 0:
                run_stage(1, k - 1)
        run_stage(1, NCH - 1)
        with scope("G_bt"):
            lax.fori_loop(0, NV // 64, cell_rows, 0)
        for n in range(2, len(stages)):
            for k in range(NCH):
                run_stage(n, k)

        with scope("H_expand"):
            for half in range(2):
                c_hi, c_lo = split(corr[:, half * 256 : (half + 1) * 256])
                for kt in range(TILES // 2):
                    rows = slice(kt * 256, (kt + 1) * 256)
                    cut = slice(PAD + kt * 256, PAD + (kt + 1) * 256)
                    add = dot3(bt_h[rows, :], bt_l[rows, :], c_hi, c_lo, NN)
                    fa[2 * half, cut, :] += add[:, :LANES]
                    fa[2 * half + 1, cut, :] += add[:, LANES:]
            edges(fa)

        with scope('H_sent'):
            for o in range(1, 8):
                coef_copy(o).wait_send()
            for k in range(NCH):
                core_copy(k).wait_send()
                gc_copy(k).wait_send()
                for group in (z1_copies(k), z2_copies(k), g2_copies(k), g1_copies(k)):
                    for cp in group:
                        cp.wait_send()
                for o in range(1, 16):
                    plane_copy(k, o).wait_send()
                    back_copy(k, o).wait_send()


    def two_steps(i, _):
        @pl.when(i == PRE // 2)
        def _():
            correct()

        with scope("E_step"):
            for src, dst, s in ((fa, fb, 2 * i), (fb, fa, 2 * i + 1)):
                on = (lev_x + (PRE - 3) > s) | (s >= PRE)
                step(src, dst, jnp.where(on, 1.0, 0.0).astype(F32))
        return 0

    lax.fori_loop(0, (PRE + POST) // 2, two_steps, 0)

    with scope("J_turn"):
        low, high = LEAD // SPAN, (LEAD + ROWS) // SPAN

        def turn_out(t, _):
            for q in range(SPAN):
                tile = fa[q, pl.ds(pl.multiple_of(PAD + t * LANES, 8), LANES), :].T
                cells[t, pl.ds(LEAD + q, high - low, stride=SPAN), :] = tile[low:high]
            out_ref[0, :, pl.ds(pl.multiple_of(t * LANES, LANES), LANES)] = cells[t, LEAD : LEAD + ROWS, :]
            return 0

        lax.fori_loop(0, TILES, turn_out, 0, unroll=4)


def body(densities, levels, coeffs):
    dma = pltpu.SemaphoreType.DMA
    vmem = pltpu.VMEM
    return pl.pallas_call(
        kernel,
        out_shape=pltpu.VMEM((1, ROWS, NV), F32),
        in_specs=[
            pl.BlockSpec(memory_space=pltpu.SMEM),
            pl.BlockSpec(memory_space=pltpu.SMEM),
            pl.BlockSpec(memory_space=pl.ANY),
        ],
        out_specs=pl.BlockSpec(memory_space=pltpu.VMEM),
        scratch_shapes=[
            vmem((TILES, WIDE, LANES), F32),
            vmem((SPAN, NV + 2 * PAD, LANES), F32),
            vmem((SPAN, NV + 2 * PAD, LANES), F32),
            vmem((WIDE, MX), BF16),
            vmem((WIDE, MX), BF16),
            vmem((MV, NV), BF16),
            vmem((MV, NV), BF16),
            vmem((NV, MV), BF16),
            vmem((NV, MV), BF16),
            vmem((MV, WIDE), BF16),
            vmem((MV, WIDE), BF16),
            vmem((MV, MX), F32),
            vmem((NCH, 128, KC), F32),
            vmem((NCH, 128, KC), F32),
            vmem((NCH, 2, 32, KC), F32),
            vmem((NCH, 2, 32, KC), F32),
            vmem((NCH, 2, 16, KC), F32),
            vmem((NCH, 32, KC), F32),
            vmem((NCH, 16, 8, KQ), F32),
            vmem((NCH, 8, 8, KQ), F32),
            vmem((MV, MX), F32),
            vmem((MV, WIDE), F32),
            vmem((8, LANES), F32),
            vmem((8, 8, LANES), F32),
            dma((TILES,)),
            dma((TILES,)),
            dma((2,)),
            dma((2,)),
            dma((8,)),
            dma((8,)),
            dma((NCH,)),
            dma((NCH,)),
            dma((NCH, 2)),
            dma((NCH, 2)),
            dma((NCH, 2)),
            dma((NCH, 2)),
            dma((NCH, 16)),
            dma((NCH, 16)),
            dma((NCH, 16)),
            dma((NCH, 16)),
            dma((NCH, 2)),
            dma((NCH, 2)),
            dma((NCH, 2)),
            dma((NCH, 2)),
            dma((NCH,)),
            dma((NCH,)),
        ],
        compiler_params=pltpu.CompilerParams(
            collective_id=0, has_side_effects=True, vmem_limit_bytes=60 * 1024 * 1024
        ),
        name="window",
    )(levels, coeffs, densities)


def solution(mesh):
    placed = (P("comp", "dom", None), P("comp", None), P("comp"))
    return jax.shard_map(
        body, mesh=mesh, in_specs=placed, out_specs=P("comp", "dom", None), check_vma=False
    )
```

```python
import functools

import jax
import jax.numpy as jnp
import numpy as np
from jax import lax
from jax.experimental import pallas as pl
from jax.experimental.pallas import tpu as pltpu
from jax.sharding import PartitionSpec as P

MX = 2048
MV = 256
PRE = 8
POST = 2
NV = 2048
ROWS = 384
NX = 6144
LANES = 128
TILES = NV // LANES
HALO = 16
SPAN = 4
LEAD = 32
USED = 112
WIDE = SPAN * LANES
PAD = 8
PLAIN = 2
EARLY = 3
NCH = 4
KC = MX // NCH
KQ = KC // 4
MESH = pl.DeviceIdType.MESH
F32 = jnp.float32
BF16 = jnp.bfloat16

TWO_PI_HI = float(np.float32(6.28125))
TWO_PI_LO = float(np.float32(2.0 * np.pi - 6.28125))
INV_TWO_PI = float(np.float32(1.0 / (2.0 * np.pi)))


def sine_terms():
    count = 6
    nodes = np.cos(np.pi * (np.arange(64) + 0.5) / 128)
    r = np.pi * nodes
    u = r * r
    basis = np.stack([u**i for i in range(count)], axis=1)
    target = np.sqrt(2.0) * np.sin(r / 2) / r
    terms, *_ = np.linalg.lstsq(basis * r[:, None], target * r, rcond=None)
    return [float(np.float32(t)) for t in terms]


SINE_TERMS = sine_terms()


def cosine(phase):
    turns = jnp.round(phase * INV_TWO_PI)
    r = (phase - turns * TWO_PI_HI) - turns * TWO_PI_LO
    u = r * r
    s = jnp.full_like(u, SINE_TERMS[-1])
    for term in SINE_TERMS[-2::-1]:
        s = s * u + term
    s = s * r
    return 1.0 - s * s


def split(x):
    hi = x.astype(BF16)
    return hi, (x - hi.astype(F32)).astype(BF16)


scope = jax.named_scope


def dot3(a_hi, a_lo, b_hi, b_lo, dims):
    def dot(a, b):
        return lax.dot_general(a, b, (dims, ((), ())), preferred_element_type=F32)

    return dot(a_hi, b_hi) + dot(a_hi, b_lo) + dot(a_lo, b_hi)


NN = ((1,), (0,))
NT = ((1,), (1,))


def kernel(
    lev_ref,
    coef_ref,
    dens_ref,
    out_ref,
    cells,
    fa,
    fb,
    bx_h,
    bx_l,
    bv_h,
    bv_l,
    bt_h,
    bt_l,
    red_h,
    red_l,
    part,
    core_in,
    core_sum,
    z1_in,
    z1_sum,
    z2_in,
    block,
    plane_in,
    back_out,
    upd,
    corr,
    coef_own,
    coef_all,
    in_sem,
    out_sem,
    halo_send,
    halo_recv,
    coef_send,
    coef_recv,
    core_send,
    core_recv,
    z1_send,
    z1_recv,
    z2_send,
    z2_recv,
    plane_send,
    plane_recv,
    back_send,
    back_recv,
    g2_send,
    g2_recv,
    g1_send,
    g1_recv,
    gc_send,
    gc_recv,
):
    c = lax.axis_index("comp")
    d = lax.axis_index("dom")
    z = d // 4
    xh = (d // 2) % 2
    core = d % 2
    p = c * 2 + xh
    nxt = (d + 1) % 16
    prv = (d + 15) % 16
    peer = d + 1 - 2 * core
    za = (z + 1 - 2 * (z % 2)) * 4 + d % 4
    zb = (3 - z) * 4 + d % 4
    s1 = (z % 2 + z // 2) % 2
    s2 = z // 2
    t1 = z // 2
    t2 = s1

    def dom_id(dom):
        return {"comp": c, "dom": dom}

    def plane_id(q):
        return {"comp": q // 2, "dom": z * 4 + (q % 2) * 2 + core}

    barrier = pltpu.get_barrier_semaphore()
    for dom in (nxt, prv, peer, za, zb):
        pl.semaphore_signal(barrier, inc=1, device_id=dom_id(dom), device_id_type=MESH)
    for o in range(1, 16):
        q = (p + o) % 16
        pl.semaphore_signal(barrier, inc=1, device_id=plane_id(q), device_id_type=MESH)

    def load(t):
        return pltpu.make_async_copy(
            dens_ref.at[0, :, pl.ds(t * LANES, LANES)],
            cells.at[t, pl.ds(LEAD, ROWS), :],
            in_sem.at[t],
        )

    for t in range(TILES):
        load(t).start()

    lev_x = lev_ref[0, 0]
    lev_v = lev_ref[0, 1]
    courant = 0.3 + lev_x.astype(F32) / 15.0
    diffusion = 0.1 + lev_v.astype(F32) / 30.0
    coef_own[...] = jnp.full((8, LANES), coef_ref[0].astype(F32), F32)
    coef_all[c] = coef_own[...]

    def power(level):
        return jnp.where(level == 0, 8.0, jnp.where(level == 1, 4.0, jnp.where(level == 2, 2.0, 1.0))).astype(F32)

    lane = lax.broadcasted_iota(jnp.int32, (16, LANES), 1)
    row16 = lax.broadcasted_iota(jnp.int32, (16, LANES), 0)

    def mode_rows(i, _):
        mode = (row16 + i * 16).astype(F32)
        r0 = pl.multiple_of(i * 16, 16)
        for t in range(TILES):
            cell = (lane + t * LANES).astype(F32)
            phase = ((np.float32(np.pi) * (cell + 0.5)) * mode) * np.float32(1.0 / NV)
            hi, lo = split(cosine(phase))
            bv_h[pl.ds(r0, 16), t * LANES : (t + 1) * LANES] = hi
            bv_l[pl.ds(r0, 16), t * LANES : (t + 1) * LANES] = lo
        return 0

    def turn_basis(t, _):
        cols = pl.ds(pl.multiple_of(t * LANES, LANES), LANES)
        bt_h[cols, :] = bv_h[:, cols].T
        bt_l[cols, :] = bv_l[:, cols].T
        return 0

    def space_basis(k, i):
        plane, first = i // (USED // 16), (i % (USED // 16)) * 16
        local = (row16 + first) * SPAN + plane - LEAD
        cell = local + d * ROWS
        cell = jnp.where(cell < 0, cell + NX, cell)
        cell = jnp.where(cell >= NX, cell - NX, cell)
        angle = np.float32(np.pi) * (cell.astype(F32) + 0.5)
        r0 = pl.multiple_of(plane * LANES + first, 16)
        for t in range(k * KC // LANES, (k + 1) * KC // LANES):
            mode = (lane + t * LANES).astype(F32)
            phase = (angle * mode) * np.float32(1.0 / NX)
            hi, lo = split(cosine(phase))
            bx_h[pl.ds(r0, 16), t * LANES : (t + 1) * LANES] = hi
            bx_l[pl.ds(r0, 16), t * LANES : (t + 1) * LANES] = lo

    def fill_space_basis(k):
        def run(i, _):
            space_basis(k, 2 * i)
            space_basis(k, 2 * i + 1)
            return 0

        lax.fori_loop(0, SPAN * USED // 32, run, 0)
        for q in range(SPAN):
            rest = slice(q * LANES + USED, (q + 1) * LANES)
            cols = slice(k * KC, (k + 1) * KC)
            bx_h[rest, cols] = jnp.zeros((LANES - USED, KC), BF16)
            bx_l[rest, cols] = jnp.zeros((LANES - USED, KC), BF16)

    with scope("A_bv"):
        lax.fori_loop(0, MV // 16, mode_rows, 0)

    with scope('B_barrier'):
        for t in range(TILES):
            load(t).wait()
        pl.semaphore_wait(barrier, 20)

    halo_up = pltpu.make_async_remote_copy(
        src_ref=cells.at[pl.ds(0, 9), pl.ds(LEAD, HALO), :],
        dst_ref=cells.at[pl.ds(0, 9), pl.ds(LEAD + ROWS, HALO), :],
        send_sem=halo_send.at[0],
        recv_sem=halo_recv.at[0],
        device_id=dom_id(prv),
        device_id_type=MESH,
    )
    halo_down = pltpu.make_async_remote_copy(
        src_ref=cells.at[pl.ds(7, 9), pl.ds(LEAD + ROWS - HALO, HALO), :],
        dst_ref=cells.at[pl.ds(7, 9), pl.ds(LEAD - HALO, HALO), :],
        send_sem=halo_send.at[1],
        recv_sem=halo_recv.at[1],
        device_id=dom_id(nxt),
        device_id_type=MESH,
    )
    halo_up.start()
    halo_down.start()

    def coef_copy(o):
        return pltpu.make_async_remote_copy(
            src_ref=coef_own,
            dst_ref=coef_all.at[c],
            send_sem=coef_send.at[o],
            recv_sem=coef_recv.at[o],
            device_id={"comp": (c + o) % 8, "dom": d},
            device_id_type=MESH,
        )

    for o in range(1, 8):
        coef_copy(o).start()

    with scope("C_bx"):
        for k in range(EARLY):
            fill_space_basis(k)

    def edges(dst):
        for q in range(SPAN):
            dst[q, PAD - 1 : PAD, :] = dst[q, PAD : PAD + 1, :]
            dst[q, PAD + NV : PAD + NV + 1, :] = dst[q, PAD + NV - 1 : PAD + NV, :]

    row_v = lax.broadcasted_iota(jnp.int32, (16, LANES), 0)
    offsets = (2.0 * row_v.astype(F32) + 1.0) / NV - 1.0

    def step(src, dst, active, scale, unit):
        share = 1.0 / diffusion if unit else scale
        rate = active * diffusion * share
        keep = share - 2.0 * rate
        pace = active * courant * share

        def part_of(first, upper):
            r = first + PAD
            velocity = offsets + first * (2.0 / NV)
            be = velocity * (pace if upper else -pace)
            al = keep - be
            f = [src[q, r : r + 16, :] for q in range(SPAN)]
            if upper:
                shifted = [pltpu.roll(f[SPAN - 1], 1, 1)] + f[:-1]
            else:
                shifted = f[1:] + [pltpu.roll(f[0], LANES - 1, 1)]
            for q in range(SPAN):
                pair = src[q, r - 1 : r + 15, :] + src[q, r + 1 : r + 17, :]
                if not unit:
                    pair = rate * pair
                dst[q, r : r + 16, :] = al * f[q] + be * shifted[q] + pair

        for first in range(0, NV, 16):
            part_of(first, first >= NV // 2)
        edges(dst)

    with scope('D_halo'):
        halo_up.wait_recv()
        halo_down.wait_recv()
        halo_up.wait_send()
        halo_down.wait_send()
    with scope("E_turn"):

        def turn_in(t, _):
            for q in range(SPAN):
                tile = cells[t, pl.ds(q, LANES, stride=SPAN), :]
                fa[q, pl.ds(pl.multiple_of(PAD + t * LANES, 8), LANES), :] = tile.T
            return 0

        lax.fori_loop(0, TILES, turn_in, 0, unroll=4)
        edges(fa)
    def correct():
        with scope("F_reduced"):
            own_lanes = lax.broadcasted_iota(jnp.int32, (MV, 2 * LANES), 1) % LANES
            own_lanes = (own_lanes >= LEAD // SPAN) & (own_lanes < (LEAD + ROWS) // SPAN)
            for half in range(2):
                reduced = jnp.zeros((MV, 2 * LANES), F32)
                for kt in range(TILES // 2):
                    cut = slice(PAD + kt * 256, PAD + (kt + 1) * 256)
                    cols = slice(kt * 256, (kt + 1) * 256)
                    f = jnp.concatenate([fa[2 * half, cut, :], fa[2 * half + 1, cut, :]], axis=1)
                    f_hi, f_lo = split(f)
                    reduced = reduced + dot3(bv_h[:, cols], bv_l[:, cols], f_hi, f_lo, NN)
                hi, lo = split(jnp.where(own_lanes, reduced, 0.0))
                red_h[:, half * 256 : (half + 1) * 256] = hi
                red_l[:, half * 256 : (half + 1) * 256] = lo

        def rows_of(base, size):
            return pl.ds(pl.multiple_of(base, size), size)

        def copy(src_ref, dst_ref, send, recv, dev):
            return pltpu.make_async_remote_copy(
                src_ref=src_ref, dst_ref=dst_ref, send_sem=send, recv_sem=recv, device_id=dev, device_id_type=MESH
            )

        def cols_of(k):
            return slice(k * KC, (k + 1) * KC)

        def core_copy(k):
            return copy(
                part.at[rows_of((1 - core) * 128, 128), pl.ds(k * KC, KC)],
                core_in.at[k],
                core_send.at[k],
                core_recv.at[k],
                dom_id(peer),
            )

        def z1_copies(k):
            return (
                copy(
                    core_sum.at[k, rows_of((1 - s1) * 32, 32), :],
                    z1_in.at[k, 0],
                    z1_send.at[k, 0],
                    z1_recv.at[k, 0],
                    dom_id(za),
                ),
                copy(
                    core_sum.at[k, rows_of(64 + (1 - t1) * 32, 32), :],
                    z1_in.at[k, 1],
                    z1_send.at[k, 1],
                    z1_recv.at[k, 1],
                    dom_id(zb),
                ),
            )

        def z2_copies(k):
            return (
                copy(
                    z1_sum.at[k, 0, rows_of((1 - s2) * 16, 16), :],
                    z2_in.at[k, 0],
                    z2_send.at[k, 0],
                    z2_recv.at[k, 0],
                    dom_id(zb),
                ),
                copy(
                    z1_sum.at[k, 1, rows_of((1 - t2) * 16, 16), :],
                    z2_in.at[k, 1],
                    z2_send.at[k, 1],
                    z2_recv.at[k, 1],
                    dom_id(za),
                ),
            )

        row_1 = core * 128 + s1 * 32 + s2 * 16
        row_2 = core * 128 + 64 + t1 * 32 + t2 * 16

        def plane_copy(k, o):
            q = (p + o) % 16
            return copy(
                block.at[k, rows_of((q // 4) * 8, 8), pl.ds(pl.multiple_of((q % 4) * KQ, KQ), KQ)],
                plane_in.at[k, o],
                plane_send.at[k, o],
                plane_recv.at[k, o],
                plane_id(q),
            )

        my_tile = p // 4
        half = my_tile // 2
        own_row = row_1 + half * (row_2 - row_1) + (my_tile % 2) * 8
        own_lane = (p % 4) * KQ

        def own_tile(k):
            return (rows_of(own_row, 8), pl.ds(pl.multiple_of(k * KC + own_lane, KQ), KQ))

        def back_copy(k, o):
            q = (p + o) % 16
            return copy(
                back_out.at[k, q // 2],
                upd.at[own_tile(k)],
                back_send.at[k, o],
                back_recv.at[k, o],
                plane_id(q),
            )

        def back_wait(k, o):
            q = (p + 16 - o) % 16
            tile = q // 4
            row = row_1 + (tile // 2) * (row_2 - row_1) + (tile % 2) * 8
            dst = upd.at[rows_of(row, 8), pl.ds(pl.multiple_of(k * KC + (q % 4) * KQ, KQ), KQ)]
            copy(back_out.at[k, 0], dst, back_send.at[k, o], back_recv.at[k, o], plane_id(q)).wait_recv()

        def g2_copies(k):
            a = upd.at[rows_of(row_1, 16), pl.ds(k * KC, KC)]
            b = upd.at[rows_of(row_2, 16), pl.ds(k * KC, KC)]
            return (
                copy(a, a, g2_send.at[k, 0], g2_recv.at[k, 0], dom_id(zb)),
                copy(b, b, g2_send.at[k, 1], g2_recv.at[k, 1], dom_id(za)),
            )

        def g2_waits(k):
            a = upd.at[rows_of(core * 128 + s1 * 32 + (1 - s2) * 16, 16), pl.ds(k * KC, KC)]
            b = upd.at[rows_of(core * 128 + 64 + t1 * 32 + (1 - t2) * 16, 16), pl.ds(k * KC, KC)]
            copy(a, a, g2_send.at[k, 0], g2_recv.at[k, 0], dom_id(zb)).wait_recv()
            copy(b, b, g2_send.at[k, 1], g2_recv.at[k, 1], dom_id(za)).wait_recv()

        def g1_copies(k):
            a = upd.at[rows_of(core * 128 + s1 * 32, 32), pl.ds(k * KC, KC)]
            b = upd.at[rows_of(core * 128 + 64 + t1 * 32, 32), pl.ds(k * KC, KC)]
            return (
                copy(a, a, g1_send.at[k, 0], g1_recv.at[k, 0], dom_id(za)),
                copy(b, b, g1_send.at[k, 1], g1_recv.at[k, 1], dom_id(zb)),
            )

        def g1_waits(k):
            a = upd.at[rows_of(core * 128 + (1 - s1) * 32, 32), pl.ds(k * KC, KC)]
            b = upd.at[rows_of(core * 128 + 64 + (1 - t1) * 32, 32), pl.ds(k * KC, KC)]
            copy(a, a, g1_send.at[k, 0], g1_recv.at[k, 0], dom_id(za)).wait_recv()
            copy(b, b, g1_send.at[k, 1], g1_recv.at[k, 1], dom_id(zb)).wait_recv()

        def gc_copy(k):
            a = upd.at[rows_of(core * 128, 128), pl.ds(k * KC, KC)]
            return copy(a, a, gc_send.at[k], gc_recv.at[k], dom_id(peer))

        def gc_wait(k):
            a = upd.at[rows_of((1 - core) * 128, 128), pl.ds(k * KC, KC)]
            copy(a, a, gc_send.at[k], gc_recv.at[k], dom_id(peer)).wait_recv()

        fac_x = power(lev_x)
        fac_v = power(lev_v)

        def stage_project(k):
            part[:, cols_of(k)] = dot3(red_h[...], red_l[...], bx_h[:, cols_of(k)], bx_l[:, cols_of(k)], NN)
            core_copy(k).start()

        def stage_core(k):
            core_copy(k).wait_recv()
            core_sum[k] = part[rows_of(core * 128, 128), cols_of(k)] + core_in[k]
            for cp in z1_copies(k):
                cp.start()

        def stage_z1(k):
            for cp in z1_copies(k):
                cp.wait_recv()
            z1_sum[k, 0] = core_sum[k, rows_of(s1 * 32, 32), :] + z1_in[k, 0]
            z1_sum[k, 1] = core_sum[k, rows_of(64 + t1 * 32, 32), :] + z1_in[k, 1]
            for cp in z2_copies(k):
                cp.start()

        def stage_z2(k):
            for cp in z2_copies(k):
                cp.wait_recv()
            for h, (keep, base) in enumerate(((s2, row_1), (t2, row_2))):
                total = z1_sum[k, h, rows_of(keep * 16, 16), :] + z2_in[k, h]
                mode_x = (lax.broadcasted_iota(jnp.int32, (16, KC), 1) + k * KC).astype(F32)
                mode_v = (lax.broadcasted_iota(jnp.int32, (16, KC), 0) + base).astype(F32)
                bend_x = mode_x * fac_x * (1.0 / MX)
                bend_v = mode_v * fac_v * (1.0 / MV)
                weight = 1.0 / ((1.0 + bend_x * bend_x) * (1.0 + bend_v * bend_v))
                scale_x = jnp.where(mode_x == 0.0, 1.0 / NX, 2.0 / NX).astype(F32)
                scale_v = jnp.where(mode_v == 0.0, 1.0 / NV, 2.0 / NV).astype(F32)
                block[k, h * 16 : (h + 1) * 16, :] = total * (weight * (scale_x * scale_v))
            for o in range(1, 16):
                plane_copy(k, o).start()

        def stage_plane(k):
            mine = block[k, rows_of((p // 4) * 8, 8), pl.ds(pl.multiple_of((p % 4) * KQ, KQ), KQ)]
            plane_in[k, 0] = mine
            for o in range(1, 16):
                plane_copy(k, o).wait_recv()
            if k == 0:
                for o in range(1, 8):
                    copy(
                        coef_own, coef_all.at[(c + 8 - o) % 8], coef_send.at[o], coef_recv.at[o], {"comp": c, "dom": d}
                    ).wait_recv()
            own = []
            for g in range(8):
                a = plane_in[k, (p + 16 - 2 * g) % 16]
                b = plane_in[k, (p + 16 - 2 * g - 1) % 16]
                own.append(a + b)
            total = jnp.zeros((8, KQ), F32)
            for g in range(8):
                total = total + coef_all[g][:, 0:1] * own[g]
            for g in range(8):
                back_out[k, g] = total - own[g]
            upd[own_tile(k)] = back_out[k, c]
            for o in range(1, 16):
                back_copy(k, o).start()

        def stage_back(k):
            for o in range(1, 16):
                back_wait(k, o)
            for cp in g2_copies(k):
                cp.start()

        def stage_g2(k):
            g2_waits(k)
            for cp in g1_copies(k):
                cp.start()

        def stage_g1(k):
            g1_waits(k)
            gc_copy(k).start()

        def stage_gc(k):
            gc_wait(k)
            u_hi, u_lo = split(upd[:, cols_of(k)])
            term = dot3(u_hi, u_lo, bx_h[:, cols_of(k)], bx_l[:, cols_of(k)], NT)
            if k == 0:
                corr[...] = term
            else:
                corr[...] += term

        stages = (stage_project, stage_core, stage_z1, stage_z2, stage_plane, stage_back, stage_g2, stage_g1, stage_gc)
        def run_stage(n, k):
            with scope("G_%d_%s" % (k, stages[n].__name__)):
                stages[n](k)

        for k in range(NCH):
            if k >= EARLY:
                fill_space_basis(k)
            run_stage(0, k)
            if k > 0:
                run_stage(1, k - 1)
        run_stage(1, NCH - 1)
        with scope("G_bt"):
            lax.fori_loop(0, TILES, turn_basis, 0, unroll=4)
        for n in range(2, len(stages) - 2):
            for k in range(NCH):
                run_stage(n, k)
        for k in range(NCH):
            run_stage(len(stages) - 2, k)
            if k > 1:
                run_stage(len(stages) - 1, k - 2)
        for k in range(NCH - 2, NCH):
            run_stage(len(stages) - 1, k)

        with scope("H_expand"):
            for half in range(2):
                c_hi, c_lo = split(corr[:, half * 256 : (half + 1) * 256])
                for kt in range(TILES // 2):
                    rows = slice(kt * 256, (kt + 1) * 256)
                    cut = slice(PAD + kt * 256, PAD + (kt + 1) * 256)
                    add = dot3(bt_h[rows, :], bt_l[rows, :], c_hi, c_lo, NN)
                    fa[2 * half, cut, :] += add[:, :LANES]
                    fa[2 * half + 1, cut, :] += add[:, LANES:]
            edges(fa)

        with scope('H_sent'):
            for o in range(1, 8):
                coef_copy(o).wait_send()
            for k in range(NCH):
                core_copy(k).wait_send()
                gc_copy(k).wait_send()
                for group in (z1_copies(k), z2_copies(k), g2_copies(k), g1_copies(k)):
                    for cp in group:
                        cp.wait_send()
                for o in range(1, 16):
                    plane_copy(k, o).wait_send()
                    back_copy(k, o).wait_send()


    def two_steps(i, _):
        @pl.when(i == PRE // 2)
        def _():
            correct()

        with scope("E_step"):
            for src, dst, s in ((fa, fb, 2 * i), (fb, fa, 2 * i + 1)):
                on = (lev_x + (PRE - 3) > s) | (s >= PRE)
                scale = jnp.where(s == 2 * PLAIN, rescale, 1.0) if dst is fb else 1.0
                step(src, dst, jnp.where(on, 1.0, 0.0).astype(F32), scale, False)
        return 0

    def two_plain(i, _):
        with scope("E_step"):
            step(fa, fb, 1.0, 1.0, True)
            step(fb, fa, 1.0, 1.0, True)
        return 0

    rescale = (diffusion * diffusion) * (diffusion * diffusion)
    lax.fori_loop(0, PLAIN, two_plain, 0)
    lax.fori_loop(PLAIN, (PRE + POST) // 2, two_steps, 0)

    with scope("J_turn"):
        low, high = LEAD // SPAN, (LEAD + ROWS) // SPAN

        def turn_out(t, _):
            for q in range(SPAN):
                tile = fa[q, pl.ds(pl.multiple_of(PAD + t * LANES, 8), LANES), :].T
                cells[t, pl.ds(LEAD + q, high - low, stride=SPAN), :] = tile[low:high]
            out_ref[0, :, pl.ds(pl.multiple_of(t * LANES, LANES), LANES)] = cells[t, LEAD : LEAD + ROWS, :]
            return 0

        lax.fori_loop(0, TILES, turn_out, 0, unroll=4)


def body(densities, levels, coeffs):
    dma = pltpu.SemaphoreType.DMA
    vmem = pltpu.VMEM
    return pl.pallas_call(
        kernel,
        out_shape=pltpu.VMEM((1, ROWS, NV), F32),
        in_specs=[
            pl.BlockSpec(memory_space=pltpu.SMEM),
            pl.BlockSpec(memory_space=pltpu.SMEM),
            pl.BlockSpec(memory_space=pl.ANY),
        ],
        out_specs=pl.BlockSpec(memory_space=pltpu.VMEM),
        scratch_shapes=[
            vmem((TILES, WIDE, LANES), F32),
            vmem((SPAN, NV + 2 * PAD, LANES), F32),
            vmem((SPAN, NV + 2 * PAD, LANES), F32),
            vmem((WIDE, MX), BF16),
            vmem((WIDE, MX), BF16),
            vmem((MV, NV), BF16),
            vmem((MV, NV), BF16),
            vmem((NV, MV), BF16),
            vmem((NV, MV), BF16),
            vmem((MV, WIDE), BF16),
            vmem((MV, WIDE), BF16),
            vmem((MV, MX), F32),
            vmem((NCH, 128, KC), F32),
            vmem((NCH, 128, KC), F32),
            vmem((NCH, 2, 32, KC), F32),
            vmem((NCH, 2, 32, KC), F32),
            vmem((NCH, 2, 16, KC), F32),
            vmem((NCH, 32, KC), F32),
            vmem((NCH, 16, 8, KQ), F32),
            vmem((NCH, 8, 8, KQ), F32),
            vmem((MV, MX), F32),
            vmem((MV, WIDE), F32),
            vmem((8, LANES), F32),
            vmem((8, 8, LANES), F32),
            dma((TILES,)),
            dma((TILES,)),
            dma((2,)),
            dma((2,)),
            dma((8,)),
            dma((8,)),
            dma((NCH,)),
            dma((NCH,)),
            dma((NCH, 2)),
            dma((NCH, 2)),
            dma((NCH, 2)),
            dma((NCH, 2)),
            dma((NCH, 16)),
            dma((NCH, 16)),
            dma((NCH, 16)),
            dma((NCH, 16)),
            dma((NCH, 2)),
            dma((NCH, 2)),
            dma((NCH, 2)),
            dma((NCH, 2)),
            dma((NCH,)),
            dma((NCH,)),
        ],
        compiler_params=pltpu.CompilerParams(
            collective_id=0, has_side_effects=True, vmem_limit_bytes=60 * 1024 * 1024
        ),
        name="window",
    )(levels, coeffs, densities)


def solution(mesh):
    placed = (P("comp", "dom", None), P("comp", None), P("comp"))
    return jax.shard_map(
        body, mesh=mesh, in_specs=placed, out_specs=P("comp", "dom", None), check_vma=False
    )
```

```python
import functools

import jax
import jax.numpy as jnp
import numpy as np
from jax import lax
from jax.experimental import pallas as pl
from jax.experimental.pallas import tpu as pltpu
from jax.sharding import PartitionSpec as P

MX = 2048
MV = 256
PRE = 8
POST = 2
NV = 2048
ROWS = 384
NX = 6144
LANES = 128
TILES = NV // LANES
HALO = 16
SPAN = 4
LEAD = 32
USED = 112
WIDE = SPAN * LANES
PAD = 8
PLAIN = 2
EARLY = 3
NCH = 4
KC = MX // NCH
KQ = KC // 4
MESH = pl.DeviceIdType.MESH
F32 = jnp.float32
BF16 = jnp.bfloat16

TWO_PI_HI = float(np.float32(6.28125))
TWO_PI_LO = float(np.float32(2.0 * np.pi - 6.28125))
INV_TWO_PI = float(np.float32(1.0 / (2.0 * np.pi)))


def sine_terms():
    count = 6
    nodes = np.cos(np.pi * (np.arange(64) + 0.5) / 128)
    r = np.pi * nodes
    u = r * r
    basis = np.stack([u**i for i in range(count)], axis=1)
    target = np.sqrt(2.0) * np.sin(r / 2) / r
    terms, *_ = np.linalg.lstsq(basis * r[:, None], target * r, rcond=None)
    return [float(np.float32(t)) for t in terms]


SINE_TERMS = sine_terms()


def cosine(phase):
    turns = jnp.round(phase * INV_TWO_PI)
    r = (phase - turns * TWO_PI_HI) - turns * TWO_PI_LO
    u = r * r
    s = jnp.full_like(u, SINE_TERMS[-1])
    for term in SINE_TERMS[-2::-1]:
        s = s * u + term
    s = s * r
    return 1.0 - s * s


def split(x):
    hi = x.astype(BF16)
    return hi, (x - hi.astype(F32)).astype(BF16)


scope = jax.named_scope


def dot3(a_hi, a_lo, b_hi, b_lo, dims):
    def dot(a, b):
        return lax.dot_general(a, b, (dims, ((), ())), preferred_element_type=F32)

    return dot(a_hi, b_hi) + dot(a_hi, b_lo) + dot(a_lo, b_hi)


NN = ((1,), (0,))
NT = ((1,), (1,))


def kernel(
    lev_ref,
    coef_ref,
    dens_ref,
    out_ref,
    cells,
    fa,
    fb,
    bx_h,
    bx_l,
    bv_h,
    bv_l,
    bt_h,
    bt_l,
    red_h,
    red_l,
    part,
    core_in,
    core_sum,
    z1_in,
    z1_sum,
    z2_in,
    block,
    plane_in,
    back_out,
    upd,
    corr,
    coef_own,
    coef_all,
    in_sem,
    out_sem,
    halo_send,
    halo_recv,
    coef_send,
    coef_recv,
    core_send,
    core_recv,
    z1_send,
    z1_recv,
    z2_send,
    z2_recv,
    plane_send,
    plane_recv,
    back_send,
    back_recv,
    g2_send,
    g2_recv,
    g1_send,
    g1_recv,
    gc_send,
    gc_recv,
):
    c = lax.axis_index("comp")
    d = lax.axis_index("dom")
    z = d // 4
    xh = (d // 2) % 2
    core = d % 2
    p = c * 2 + xh
    nxt = (d + 1) % 16
    prv = (d + 15) % 16
    peer = d + 1 - 2 * core
    za = (z + 1 - 2 * (z % 2)) * 4 + d % 4
    zb = (3 - z) * 4 + d % 4
    s1 = (z % 2 + z // 2) % 2
    s2 = z // 2
    t1 = z // 2
    t2 = s1

    def dom_id(dom):
        return {"comp": c, "dom": dom}

    def plane_id(q):
        return {"comp": q // 2, "dom": z * 4 + (q % 2) * 2 + core}

    barrier = pltpu.get_barrier_semaphore()
    for dom in (nxt, prv, peer, za, zb):
        pl.semaphore_signal(barrier, inc=1, device_id=dom_id(dom), device_id_type=MESH)
    for o in range(1, 16):
        q = (p + o) % 16
        pl.semaphore_signal(barrier, inc=1, device_id=plane_id(q), device_id_type=MESH)

    def load(t):
        return pltpu.make_async_copy(
            dens_ref.at[0, :, pl.ds(t * LANES, LANES)],
            cells.at[t, pl.ds(LEAD, ROWS), :],
            in_sem.at[t],
        )

    for t in range(TILES):
        load(t).start()

    lev_x = lev_ref[0, 0]
    lev_v = lev_ref[0, 1]
    courant = 0.3 + lev_x.astype(F32) / 15.0
    diffusion = 0.1 + lev_v.astype(F32) / 30.0
    coef_own[...] = jnp.full((8, LANES), coef_ref[0].astype(F32), F32)
    coef_all[c] = coef_own[...]

    def power(level):
        return jnp.where(level == 0, 8.0, jnp.where(level == 1, 4.0, jnp.where(level == 2, 2.0, 1.0))).astype(F32)

    lane = lax.broadcasted_iota(jnp.int32, (16, LANES), 1)
    row16 = lax.broadcasted_iota(jnp.int32, (16, LANES), 0)

    def mode_rows(i, _):
        mode = (row16 + i * 16).astype(F32)
        r0 = pl.multiple_of(i * 16, 16)
        for t in range(TILES):
            cell = (lane + t * LANES).astype(F32)
            phase = ((np.float32(np.pi) * (cell + 0.5)) * mode) * np.float32(1.0 / NV)
            hi, lo = split(cosine(phase))
            bv_h[pl.ds(r0, 16), t * LANES : (t + 1) * LANES] = hi
            bv_l[pl.ds(r0, 16), t * LANES : (t + 1) * LANES] = lo
        return 0

    def turn_basis(t, _):
        cols = pl.ds(pl.multiple_of(t * LANES, LANES), LANES)
        bt_h[cols, :] = bv_h[:, cols].T
        bt_l[cols, :] = bv_l[:, cols].T
        return 0

    def space_basis(k, i):
        plane, first = i // (USED // 16), (i % (USED // 16)) * 16
        local = (row16 + first) * SPAN + plane - LEAD
        cell = local + d * ROWS
        cell = jnp.where(cell < 0, cell + NX, cell)
        cell = jnp.where(cell >= NX, cell - NX, cell)
        angle = np.float32(np.pi) * (cell.astype(F32) + 0.5)
        r0 = pl.multiple_of(plane * LANES + first, 16)
        for t in range(k * KC // LANES, (k + 1) * KC // LANES):
            mode = (lane + t * LANES).astype(F32)
            phase = (angle * mode) * np.float32(1.0 / NX)
            hi, lo = split(cosine(phase))
            bx_h[pl.ds(r0, 16), t * LANES : (t + 1) * LANES] = hi
            bx_l[pl.ds(r0, 16), t * LANES : (t + 1) * LANES] = lo

    def fill_space_basis(k):
        def run(i, _):
            space_basis(k, 2 * i)
            space_basis(k, 2 * i + 1)
            return 0

        lax.fori_loop(0, SPAN * USED // 32, run, 0)
        for q in range(SPAN):
            rest = slice(q * LANES + USED, (q + 1) * LANES)
            cols = slice(k * KC, (k + 1) * KC)
            bx_h[rest, cols] = jnp.zeros((LANES - USED, KC), BF16)
            bx_l[rest, cols] = jnp.zeros((LANES - USED, KC), BF16)

    with scope("A_bv"):
        lax.fori_loop(0, MV // 16, mode_rows, 0)

    with scope('B_barrier'):
        for t in range(TILES):
            load(t).wait()
        pl.semaphore_wait(barrier, 20)

    halo_up = pltpu.make_async_remote_copy(
        src_ref=cells.at[pl.ds(0, 9), pl.ds(LEAD, HALO), :],
        dst_ref=cells.at[pl.ds(0, 9), pl.ds(LEAD + ROWS, HALO), :],
        send_sem=halo_send.at[0],
        recv_sem=halo_recv.at[0],
        device_id=dom_id(prv),
        device_id_type=MESH,
    )
    halo_down = pltpu.make_async_remote_copy(
        src_ref=cells.at[pl.ds(7, 9), pl.ds(LEAD + ROWS - HALO, HALO), :],
        dst_ref=cells.at[pl.ds(7, 9), pl.ds(LEAD - HALO, HALO), :],
        send_sem=halo_send.at[1],
        recv_sem=halo_recv.at[1],
        device_id=dom_id(nxt),
        device_id_type=MESH,
    )
    halo_up.start()
    halo_down.start()

    def coef_copy(o):
        return pltpu.make_async_remote_copy(
            src_ref=coef_own,
            dst_ref=coef_all.at[c],
            send_sem=coef_send.at[o],
            recv_sem=coef_recv.at[o],
            device_id={"comp": (c + o) % 8, "dom": d},
            device_id_type=MESH,
        )

    for o in range(1, 8):
        coef_copy(o).start()

    with scope("C_bx"):
        for k in range(EARLY):
            fill_space_basis(k)

    def edges(dst):
        for q in range(SPAN):
            dst[q, PAD - 1 : PAD, :] = dst[q, PAD : PAD + 1, :]
            dst[q, PAD + NV : PAD + NV + 1, :] = dst[q, PAD + NV - 1 : PAD + NV, :]

    row_v = lax.broadcasted_iota(jnp.int32, (16, LANES), 0)
    offsets = (2.0 * row_v.astype(F32) + 1.0) / NV - 1.0

    def step(src, dst, active, scale, unit):
        share = 1.0 / diffusion if unit else scale
        rate = active * diffusion * share
        keep = share - 2.0 * rate
        pace = active * courant * share

        def part_of(first, upper):
            r = first + PAD
            velocity = offsets + first * (2.0 / NV)
            be = velocity * (pace if upper else -pace)
            al = keep - be
            f = [src[q, r : r + 16, :] for q in range(SPAN)]
            if upper:
                shifted = [pltpu.roll(f[SPAN - 1], 1, 1)] + f[:-1]
            else:
                shifted = f[1:] + [pltpu.roll(f[0], LANES - 1, 1)]
            for q in range(SPAN):
                pair = src[q, r - 1 : r + 15, :] + src[q, r + 1 : r + 17, :]
                if not unit:
                    pair = rate * pair
                dst[q, r : r + 16, :] = al * f[q] + be * shifted[q] + pair

        for first in range(0, NV, 16):
            part_of(first, first >= NV // 2)
        edges(dst)

    with scope('D_halo'):
        halo_up.wait_recv()
        halo_down.wait_recv()
        halo_up.wait_send()
        halo_down.wait_send()
    with scope("E_turn"):

        def turn_in(t, _):
            for q in range(SPAN):
                tile = cells[t, pl.ds(q, LANES, stride=SPAN), :]
                fa[q, pl.ds(pl.multiple_of(PAD + t * LANES, 8), LANES), :] = tile.T
            return 0

        lax.fori_loop(0, TILES, turn_in, 0, unroll=4)
        edges(fa)
    def correct():
        with scope("F_reduced"):
            own_lanes = lax.broadcasted_iota(jnp.int32, (MV, 2 * LANES), 1) % LANES
            own_lanes = (own_lanes >= LEAD // SPAN) & (own_lanes < (LEAD + ROWS) // SPAN)
            for half in range(2):
                reduced = jnp.zeros((MV, 2 * LANES), F32)
                for kt in range(TILES // 2):
                    cut = slice(PAD + kt * 256, PAD + (kt + 1) * 256)
                    cols = slice(kt * 256, (kt + 1) * 256)
                    f = jnp.concatenate([fa[2 * half, cut, :], fa[2 * half + 1, cut, :]], axis=1)
                    f_hi, f_lo = split(f)
                    reduced = reduced + dot3(bv_h[:, cols], bv_l[:, cols], f_hi, f_lo, NN)
                hi, lo = split(jnp.where(own_lanes, reduced, 0.0))
                red_h[:, half * 256 : (half + 1) * 256] = hi
                red_l[:, half * 256 : (half + 1) * 256] = lo

        def rows_of(base, size):
            return pl.ds(pl.multiple_of(base, size), size)

        def copy(src_ref, dst_ref, send, recv, dev):
            return pltpu.make_async_remote_copy(
                src_ref=src_ref, dst_ref=dst_ref, send_sem=send, recv_sem=recv, device_id=dev, device_id_type=MESH
            )

        def cols_of(k):
            return slice(k * KC, (k + 1) * KC)

        def core_copy(k):
            return copy(
                part.at[rows_of((1 - core) * 128, 128), pl.ds(k * KC, KC)],
                core_in.at[k],
                core_send.at[k],
                core_recv.at[k],
                dom_id(peer),
            )

        def z1_copies(k):
            return (
                copy(
                    core_sum.at[k, rows_of((1 - s1) * 32, 32), :],
                    z1_in.at[k, 0],
                    z1_send.at[k, 0],
                    z1_recv.at[k, 0],
                    dom_id(za),
                ),
                copy(
                    core_sum.at[k, rows_of(64 + (1 - t1) * 32, 32), :],
                    z1_in.at[k, 1],
                    z1_send.at[k, 1],
                    z1_recv.at[k, 1],
                    dom_id(zb),
                ),
            )

        def z2_copies(k):
            return (
                copy(
                    z1_sum.at[k, 0, rows_of((1 - s2) * 16, 16), :],
                    z2_in.at[k, 0],
                    z2_send.at[k, 0],
                    z2_recv.at[k, 0],
                    dom_id(zb),
                ),
                copy(
                    z1_sum.at[k, 1, rows_of((1 - t2) * 16, 16), :],
                    z2_in.at[k, 1],
                    z2_send.at[k, 1],
                    z2_recv.at[k, 1],
                    dom_id(za),
                ),
            )

        row_1 = core * 128 + s1 * 32 + s2 * 16
        row_2 = core * 128 + 64 + t1 * 32 + t2 * 16

        def plane_copy(k, o):
            q = (p + o) % 16
            return copy(
                block.at[k, rows_of((q // 4) * 8, 8), pl.ds(pl.multiple_of((q % 4) * KQ, KQ), KQ)],
                plane_in.at[k, o],
                plane_send.at[k, o],
                plane_recv.at[k, o],
                plane_id(q),
            )

        my_tile = p // 4
        half = my_tile // 2
        own_row = row_1 + half * (row_2 - row_1) + (my_tile % 2) * 8
        own_lane = (p % 4) * KQ

        def own_tile(k):
            return (rows_of(own_row, 8), pl.ds(pl.multiple_of(k * KC + own_lane, KQ), KQ))

        def back_copy(k, o):
            q = (p + o) % 16
            return copy(
                back_out.at[k, q // 2],
                upd.at[own_tile(k)],
                back_send.at[k, o],
                back_recv.at[k, o],
                plane_id(q),
            )

        def back_wait(k, o):
            q = (p + 16 - o) % 16
            tile = q // 4
            row = row_1 + (tile // 2) * (row_2 - row_1) + (tile % 2) * 8
            dst = upd.at[rows_of(row, 8), pl.ds(pl.multiple_of(k * KC + (q % 4) * KQ, KQ), KQ)]
            copy(back_out.at[k, 0], dst, back_send.at[k, o], back_recv.at[k, o], plane_id(q)).wait_recv()

        def g2_copies(k):
            a = upd.at[rows_of(row_1, 16), pl.ds(k * KC, KC)]
            b = upd.at[rows_of(row_2, 16), pl.ds(k * KC, KC)]
            return (
                copy(a, a, g2_send.at[k, 0], g2_recv.at[k, 0], dom_id(zb)),
                copy(b, b, g2_send.at[k, 1], g2_recv.at[k, 1], dom_id(za)),
            )

        def g2_waits(k):
            a = upd.at[rows_of(core * 128 + s1 * 32 + (1 - s2) * 16, 16), pl.ds(k * KC, KC)]
            b = upd.at[rows_of(core * 128 + 64 + t1 * 32 + (1 - t2) * 16, 16), pl.ds(k * KC, KC)]
            copy(a, a, g2_send.at[k, 0], g2_recv.at[k, 0], dom_id(zb)).wait_recv()
            copy(b, b, g2_send.at[k, 1], g2_recv.at[k, 1], dom_id(za)).wait_recv()

        def g1_copies(k):
            a = upd.at[rows_of(core * 128 + s1 * 32, 32), pl.ds(k * KC, KC)]
            b = upd.at[rows_of(core * 128 + 64 + t1 * 32, 32), pl.ds(k * KC, KC)]
            return (
                copy(a, a, g1_send.at[k, 0], g1_recv.at[k, 0], dom_id(za)),
                copy(b, b, g1_send.at[k, 1], g1_recv.at[k, 1], dom_id(zb)),
            )

        def g1_waits(k):
            a = upd.at[rows_of(core * 128 + (1 - s1) * 32, 32), pl.ds(k * KC, KC)]
            b = upd.at[rows_of(core * 128 + 64 + (1 - t1) * 32, 32), pl.ds(k * KC, KC)]
            copy(a, a, g1_send.at[k, 0], g1_recv.at[k, 0], dom_id(za)).wait_recv()
            copy(b, b, g1_send.at[k, 1], g1_recv.at[k, 1], dom_id(zb)).wait_recv()

        def gc_copy(k):
            a = upd.at[rows_of(core * 128, 128), pl.ds(k * KC, KC)]
            return copy(a, a, gc_send.at[k], gc_recv.at[k], dom_id(peer))

        def gc_wait(k):
            a = upd.at[rows_of((1 - core) * 128, 128), pl.ds(k * KC, KC)]
            copy(a, a, gc_send.at[k], gc_recv.at[k], dom_id(peer)).wait_recv()

        fac_x = power(lev_x)
        fac_v = power(lev_v)

        def stage_project(k):
            part[:, cols_of(k)] = dot3(red_h[...], red_l[...], bx_h[:, cols_of(k)], bx_l[:, cols_of(k)], NN)
            core_copy(k).start()

        def stage_core(k):
            core_copy(k).wait_recv()
            core_sum[k] = part[rows_of(core * 128, 128), cols_of(k)] + core_in[k]
            for cp in z1_copies(k):
                cp.start()

        def stage_z1(k):
            for cp in z1_copies(k):
                cp.wait_recv()
            z1_sum[k, 0] = core_sum[k, rows_of(s1 * 32, 32), :] + z1_in[k, 0]
            z1_sum[k, 1] = core_sum[k, rows_of(64 + t1 * 32, 32), :] + z1_in[k, 1]
            for cp in z2_copies(k):
                cp.start()

        def stage_z2(k):
            for cp in z2_copies(k):
                cp.wait_recv()
            for h, (keep, base) in enumerate(((s2, row_1), (t2, row_2))):
                total = z1_sum[k, h, rows_of(keep * 16, 16), :] + z2_in[k, h]
                mode_x = (lax.broadcasted_iota(jnp.int32, (16, KC), 1) + k * KC).astype(F32)
                mode_v = (lax.broadcasted_iota(jnp.int32, (16, KC), 0) + base).astype(F32)
                bend_x = mode_x * fac_x * (1.0 / MX)
                bend_v = mode_v * fac_v * (1.0 / MV)
                weight = 1.0 / ((1.0 + bend_x * bend_x) * (1.0 + bend_v * bend_v))
                scale_x = jnp.where(mode_x == 0.0, 1.0 / NX, 2.0 / NX).astype(F32)
                scale_v = jnp.where(mode_v == 0.0, 1.0 / NV, 2.0 / NV).astype(F32)
                block[k, h * 16 : (h + 1) * 16, :] = total * (weight * (scale_x * scale_v))
            for o in range(1, 16):
                plane_copy(k, o).start()

        def stage_plane(k):
            mine = block[k, rows_of((p // 4) * 8, 8), pl.ds(pl.multiple_of((p % 4) * KQ, KQ), KQ)]
            plane_in[k, 0] = mine
            for o in range(1, 16):
                plane_copy(k, o).wait_recv()
            if k == 0:
                for o in range(1, 8):
                    copy(
                        coef_own, coef_all.at[(c + 8 - o) % 8], coef_send.at[o], coef_recv.at[o], {"comp": c, "dom": d}
                    ).wait_recv()
            own = []
            for g in range(8):
                a = plane_in[k, (p + 16 - 2 * g) % 16]
                b = plane_in[k, (p + 16 - 2 * g - 1) % 16]
                own.append(a + b)
            total = jnp.zeros((8, KQ), F32)
            for g in range(8):
                total = total + coef_all[g][:, 0:1] * own[g]
            for g in range(8):
                back_out[k, g] = total - own[g]
            upd[own_tile(k)] = back_out[k, c]
            for o in range(1, 16):
                back_copy(k, o).start()

        def stage_back(k):
            for o in range(1, 16):
                back_wait(k, o)
            for cp in g2_copies(k):
                cp.start()

        def stage_g2(k):
            g2_waits(k)
            for cp in g1_copies(k):
                cp.start()

        def stage_g1(k):
            g1_waits(k)
            gc_copy(k).start()

        def stage_gc(k):
            gc_wait(k)
            u_hi, u_lo = split(upd[:, cols_of(k)])
            term = dot3(u_hi, u_lo, bx_h[:, cols_of(k)], bx_l[:, cols_of(k)], NT)
            if k == 0:
                corr[...] = term
            else:
                corr[...] += term

        stages = (stage_project, stage_core, stage_z1, stage_z2, stage_plane, stage_back, stage_g2, stage_g1, stage_gc)
        def run_stage(n, k):
            with scope("G_%d_%s" % (k, stages[n].__name__)):
                stages[n](k)

        for k in range(NCH):
            if k >= EARLY:
                fill_space_basis(k)
            run_stage(0, k)
            if k > 0:
                run_stage(1, k - 1)
        with scope("G_bt"):
            lax.fori_loop(0, TILES, turn_basis, 0, unroll=4)
        run_stage(1, NCH - 1)
        for n in range(2, len(stages) - 2):
            for k in range(NCH):
                run_stage(n, k)
        for k in range(NCH):
            run_stage(len(stages) - 2, k)
            if k > 1:
                run_stage(len(stages) - 1, k - 2)
        for k in range(NCH - 2, NCH):
            run_stage(len(stages) - 1, k)

        with scope("H_expand"):
            for half in range(2):
                c_hi, c_lo = split(corr[:, half * 256 : (half + 1) * 256])
                for kt in range(TILES // 2):
                    rows = slice(kt * 256, (kt + 1) * 256)
                    cut = slice(PAD + kt * 256, PAD + (kt + 1) * 256)
                    add = dot3(bt_h[rows, :], bt_l[rows, :], c_hi, c_lo, NN)
                    fa[2 * half, cut, :] += add[:, :LANES]
                    fa[2 * half + 1, cut, :] += add[:, LANES:]
            edges(fa)

        with scope('H_sent'):
            for o in range(1, 8):
                coef_copy(o).wait_send()
            for k in range(NCH):
                core_copy(k).wait_send()
                gc_copy(k).wait_send()
                for group in (z1_copies(k), z2_copies(k), g2_copies(k), g1_copies(k)):
                    for cp in group:
                        cp.wait_send()
                for o in range(1, 16):
                    plane_copy(k, o).wait_send()
                    back_copy(k, o).wait_send()


    def two_steps(i, _):
        @pl.when(i == PRE // 2)
        def _():
            correct()

        with scope("E_step"):
            for src, dst, s in ((fa, fb, 2 * i), (fb, fa, 2 * i + 1)):
                on = (lev_x + (PRE - 3) > s) | (s >= PRE)
                scale = jnp.where(s == 2 * PLAIN, rescale, 1.0) if dst is fb else 1.0
                step(src, dst, jnp.where(on, 1.0, 0.0).astype(F32), scale, False)
        return 0

    def two_plain(i, _):
        with scope("E_step"):
            step(fa, fb, 1.0, 1.0, True)
            step(fb, fa, 1.0, 1.0, True)
        return 0

    rescale = (diffusion * diffusion) * (diffusion * diffusion)
    lax.fori_loop(0, PLAIN, two_plain, 0)
    lax.fori_loop(PLAIN, (PRE + POST) // 2, two_steps, 0)

    with scope("J_turn"):
        low, high = LEAD // SPAN, (LEAD + ROWS) // SPAN

        def turn_out(t, _):
            for q in range(SPAN):
                tile = fa[q, pl.ds(pl.multiple_of(PAD + t * LANES, 8), LANES), :].T
                cells[t, pl.ds(LEAD + q, high - low, stride=SPAN), :] = tile[low:high]
            out_ref[0, :, pl.ds(pl.multiple_of(t * LANES, LANES), LANES)] = cells[t, LEAD : LEAD + ROWS, :]
            return 0

        lax.fori_loop(0, TILES, turn_out, 0, unroll=4)


def body(densities, levels, coeffs):
    dma = pltpu.SemaphoreType.DMA
    vmem = pltpu.VMEM
    return pl.pallas_call(
        kernel,
        out_shape=pltpu.VMEM((1, ROWS, NV), F32),
        in_specs=[
            pl.BlockSpec(memory_space=pltpu.SMEM),
            pl.BlockSpec(memory_space=pltpu.SMEM),
            pl.BlockSpec(memory_space=pl.ANY),
        ],
        out_specs=pl.BlockSpec(memory_space=pltpu.VMEM),
        scratch_shapes=[
            vmem((TILES, WIDE, LANES), F32),
            vmem((SPAN, NV + 2 * PAD, LANES), F32),
            vmem((SPAN, NV + 2 * PAD, LANES), F32),
            vmem((WIDE, MX), BF16),
            vmem((WIDE, MX), BF16),
            vmem((MV, NV), BF16),
            vmem((MV, NV), BF16),
            vmem((NV, MV), BF16),
            vmem((NV, MV), BF16),
            vmem((MV, WIDE), BF16),
            vmem((MV, WIDE), BF16),
            vmem((MV, MX), F32),
            vmem((NCH, 128, KC), F32),
            vmem((NCH, 128, KC), F32),
            vmem((NCH, 2, 32, KC), F32),
            vmem((NCH, 2, 32, KC), F32),
            vmem((NCH, 2, 16, KC), F32),
            vmem((NCH, 32, KC), F32),
            vmem((NCH, 16, 8, KQ), F32),
            vmem((NCH, 8, 8, KQ), F32),
            vmem((MV, MX), F32),
            vmem((MV, WIDE), F32),
            vmem((8, LANES), F32),
            vmem((8, 8, LANES), F32),
            dma((TILES,)),
            dma((TILES,)),
            dma((2,)),
            dma((2,)),
            dma((8,)),
            dma((8,)),
            dma((NCH,)),
            dma((NCH,)),
            dma((NCH, 2)),
            dma((NCH, 2)),
            dma((NCH, 2)),
            dma((NCH, 2)),
            dma((NCH, 16)),
            dma((NCH, 16)),
            dma((NCH, 16)),
            dma((NCH, 16)),
            dma((NCH, 2)),
            dma((NCH, 2)),
            dma((NCH, 2)),
            dma((NCH, 2)),
            dma((NCH,)),
            dma((NCH,)),
        ],
        compiler_params=pltpu.CompilerParams(
            collective_id=0, has_side_effects=True, vmem_limit_bytes=60 * 1024 * 1024
        ),
        name="window",
    )(levels, coeffs, densities)


def solution(mesh):
    placed = (P("comp", "dom", None), P("comp", None), P("comp"))
    return jax.shard_map(
        body, mesh=mesh, in_specs=placed, out_specs=P("comp", "dom", None), check_vma=False
    )
```
